256 devices in a mesh: fsdp: 32 (over z, x), rep: 8 (over y, core).
Axes of the slice: x: 4, y: 4, z: 8, core: 2. Of those that a mesh axis runs over, the one named last changes fastest.
Arguments:
- partials: bfloat16 [8, 112, 1024, 1024], P('rep', None, 'fsdp'), may hold values from -400 to 400
- sketch: bfloat16 [32, 8, 2, 1024, 256], P('fsdp', 'rep'), may hold values from -3 to 3
- owner_table: int32 [112, 1], replicated, may hold values from 0 to 31; in each aligned block of 14 rows (0 to 13, 14 to 27, ...) at most 2 rows name the same one
Outputs:
- update: bfloat16 [112, 1024, 1024], P('rep', 'fsdp')
- new_sketch: bfloat16 [32, 8, 2, 1024, 256], P('fsdp', 'rep')
The draws below stay inside these ranges and needn't reach their ends.
Inputs may be any that keep to these rules, and one draw needn't show every extreme that they name: `owner_table`: in each aligned slice of 14 blocks no owner holds more than 2 blocks; some owner holds exactly 2 in some slice.
All inputs are finite; a program needn't handle non-finite values.
Results may differ from the reference program's by a relative error of at most 0.015.
Values may be sent and summed in bfloat16 or wider, within the bound.
A program may use at most 128 MiB of HBM per device.

```python
import math
import jax
import jax.numpy as jnp
import numpy as np
from jax import lax

BS = 1024
RANK = 256
SLOTS = 2
NS_ITERS = 5
BLK_REP = 14
NB = 112
N_FSDP = 32
N_REP = 8


def draw_partials(key, part):
    row_key, column_key, noise_key = jax.random.split(key, 3)
    row_scale = jnp.exp(jax.random.uniform(row_key, (NB, BS, 1), jnp.float32) * math.log(10.0))
    column_scale = jnp.exp(jax.random.uniform(column_key, (NB, 1, BS), jnp.float32) * math.log(10.0))
    block_place = jnp.arange(NB, dtype=jnp.float32) / NB
    row_place = jnp.arange(BS, dtype=jnp.float32) / BS
    trend = jnp.exp(0.5 * math.log(3.0) * (block_place[:, None, None] + row_place[None, :, None]))
    amplitude = 0.1 * row_scale * column_scale * trend

    def replica(number):
        noise = jnp.clip(jax.random.normal(jax.random.fold_in(noise_key, number), (NB, BS, BS), jnp.float32), -6.0, 6.0)
        return (amplitude * noise).astype(jnp.bfloat16)
    return lax.map(replica, jnp.arange(N_REP, dtype=jnp.int32))


def steps_of(stream_key, dims, shards, smallest, top_value):
    level, own = 1.0, jax.random.fold_in(stream_key, 6)
    for axis_at, shards_of in shards:
        steps = jnp.exp(jax.random.uniform(jax.random.fold_in(own, axis_at), (shards_of,), jnp.float32, smallest / len(shards), top_value / len(shards)))
        level = level * jnp.repeat(steps, dims[axis_at] // shards_of).reshape([-1 if axis == axis_at else 1 for axis in range(len(dims))])
    return level


def assign_block(own_key, own, number, rows, number_of, top, bound, slope):
    ranking = jax.random.permutation(own_key, number_of)
    heavy_load, ordinary = load_shares(number_of, rows * top, bound, slope, True), load_shares(number_of, rows * top, bound, slope, False)
    places = jnp.arange(number_of)

    def named(lengths, offset_by):
        used = int((lengths > 0).sum())
        fixed = max(1, used // 4)
        shifted = fixed + (places - fixed + offset_by * (used - fixed)) % max(1, number_of - fixed)
        return jnp.zeros((number_of,), jnp.int32).at[ranking[jnp.where(places < fixed, places, shifted)]].set(jnp.asarray(lengths, jnp.int32))

    lengths = jnp.where(number % 4 == 0, named(heavy_load, number // 4), named(ordinary, number - number // 4 - 1))
    mixed = jax.random.permutation(jax.random.fold_in(own, 3), number_of)
    giver, taker = mixed[0:number_of // 2 * 2:2], mixed[1:number_of // 2 * 2:2]
    slack = jnp.minimum(lengths[giver] - 1, bound - lengths[taker]) // 2
    slack = jnp.where((giver == ranking[0]) | (taker == ranking[0]) | (lengths[taker] == 0), 0, jnp.maximum(slack, 0))
    shifted = jax.random.randint(jax.random.fold_in(own, 4), (number_of // 2,), 0, 1 << 20) % (slack + 1)
    lengths = lengths.at[giver].add(-shifted).at[taker].add(shifted)
    labels = jnp.searchsorted(jnp.cumsum(lengths), jnp.arange(rows * top), side="right").astype(jnp.int32)
    grid = labels.reshape(top, rows).T
    grid = grid[jax.random.permutation(jax.random.fold_in(own, 1), rows)]
    offset_by = jax.random.randint(jax.random.fold_in(own, 2), (rows, 1), 0, top)
    return jnp.take_along_axis(grid, (jnp.arange(top)[None, :] + offset_by) % top, axis=1)


def load_shares(amount, total, reach, slope, full):
    portions = [(1 << 20) // math.isqrt(standing ** slope) + 1 for standing in range(1, amount + 1)]
    largest = reach if full else min(reach, max(-(-total // amount), total * portions[0] // sum(portions)))
    least = 1 if total - largest >= amount - 1 else 0
    holding, rest = [largest] + [least] * (amount - 1), total - largest - least * (amount - 1)
    while rest > 0:
        movable = [i for i in range(1, amount) if holding[i] < largest] or [i for i in range(1, amount) if holding[i] < reach]
        mass, remaining = sum([portions[i] for i in movable]), rest
        for i in movable:
            extra = min(reach - holding[i], max(1, remaining * portions[i] // mass), rest)
            holding[i] = holding[i] + extra
            rest = rest - extra
    return np.array(holding)


def bell_draw(own_key, shape, scale, most, cuts=(), kind=jnp.bfloat16):
    factor_of = steps_of(own_key, shape, cuts, -0.22, 0.18) if cuts else 1.0
    array = jax.random.normal(own_key, shape, jnp.float32) * scale * factor_of
    return jnp.minimum(jnp.maximum(array, -most), most).astype(kind)


def setup_inputs(seed: int = 0) -> dict:
    seeds = jax.random.split(jax.random.key(seed), 4)
    partials = draw_partials(jax.random.fold_in(seeds[3], 71), 0)
    sketch = bell_draw(seeds[1], (N_FSDP, N_REP, SLOTS, BS, RANK), 0.5, 3.0, ((0, 32), (1, 8)))
    owner_table_keys = jax.random.split(jax.random.fold_in(seeds[2], 1), NB // BLK_REP)
    owner_table_turns = jax.random.permutation(jax.random.fold_in(seeds[2], 3), NB // BLK_REP)
    owner_table = jax.vmap(lambda own, number: assign_block(jax.random.fold_in(seeds[2], 2), own, number, BLK_REP, N_FSDP, 1, SLOTS, 2))(owner_table_keys, owner_table_turns).reshape((NB, 1))
    return {"partials": partials, "sketch": sketch, "owner_table": owner_table}


DECAY = 0.9
DAMPING = 64.0
FIRST_AXES = (((0,), (0,)), ((), ()))
LAST_AXES = (((1,), (1,)), ((), ()))

def inverse_root(matrix, epsilon):
    identity = jnp.eye(matrix.shape[0], dtype=jnp.float32)
    trace_sum = jnp.trace(matrix) + epsilon
    current = matrix / trace_sum
    inverse = identity
    for repeat in range(NS_ITERS):
        middle = 1.5 * identity - 0.5 * jnp.dot(inverse, current, precision=lax.Precision.HIGHEST)
        current = jnp.dot(current, middle, precision=lax.Precision.HIGHEST)
        inverse = jnp.dot(middle, inverse, precision=lax.Precision.HIGHEST)
    return inverse / jnp.sqrt(trace_sum)

def precondition(gradient, current_sketch):
    identity = jnp.eye(current_sketch.shape[1], dtype=jnp.float32)
    projected = lax.dot_general(gradient, current_sketch, FIRST_AXES, preferred_element_type=jnp.float32).astype(jnp.bfloat16)
    gram_matrix = lax.dot_general(current_sketch, current_sketch, FIRST_AXES, preferred_element_type=jnp.float32).astype(jnp.bfloat16)
    powered = DECAY * jnp.dot(current_sketch, gram_matrix, preferred_element_type=jnp.float32) + jnp.dot(gradient, projected, preferred_element_type=jnp.float32)
    inner_gram = lax.dot_general(powered, powered, FIRST_AXES, precision=lax.Precision.HIGHEST)
    basis_full = jnp.dot(powered, inverse_root(inner_gram, 1e-06), precision=lax.Precision.HIGHEST)
    basis_low = basis_full.astype(jnp.bfloat16)
    coefficients = lax.dot_general(gradient, basis_low, FIRST_AXES, preferred_element_type=jnp.float32).astype(jnp.bfloat16)
    alignment = lax.dot_general(current_sketch, basis_low, FIRST_AXES, preferred_element_type=jnp.float32)
    energy = DECAY * lax.dot_general(alignment, alignment, FIRST_AXES, precision=lax.Precision.HIGHEST) + lax.dot_general(coefficients, coefficients, FIRST_AXES, preferred_element_type=jnp.float32)
    root_inverse = inverse_root(energy + DAMPING * identity, 0.0)
    inner_part = jnp.dot(energy, root_inverse, precision=lax.Precision.HIGHEST)
    new_block = jnp.dot(basis_full, inner_part, precision=lax.Precision.HIGHEST).astype(jnp.bfloat16)
    mix_matrix = math.sqrt(DAMPING) * root_inverse - identity
    side_terms = lax.dot_general(coefficients.astype(jnp.float32), mix_matrix, LAST_AXES, precision=lax.Precision.HIGHEST).astype(jnp.bfloat16)
    update_block = (gradient.astype(jnp.float32) + lax.dot_general(basis_low, side_terms, LAST_AXES, preferred_element_type=jnp.float32)).astype(jnp.bfloat16)
    return (update_block, new_block)

def reference(partials, sketch, owner_table):
    owner_ids = owner_table[:, 0]
    block_ids = jnp.arange(NB, dtype=jnp.int32)

    def reduce_block(block):
        replicas = lax.dynamic_index_in_dim(partials, block, axis=1, keepdims=False)
        summed = lax.optimization_barrier(jnp.sum(replicas.astype(jnp.float32), axis=0)).astype(jnp.bfloat16)
        wide = summed.astype(jnp.float32)
        return (summed, jnp.sum(wide * wide))
    gradients, squares = lax.map(reduce_block, block_ids)
    sum_squares = jnp.sum(squares)
    clip_limit = 0.5 * math.sqrt(NB * BS * BS)
    clip_factor = jnp.minimum(1.0, clip_limit / jnp.sqrt(sum_squares + 1e-06))
    slice_ids = block_ids // BLK_REP
    same_owner = (owner_ids[:, None] == owner_ids[None, :]) & (slice_ids[:, None] == slice_ids[None, :]) & (block_ids[:, None] < block_ids[None, :])
    rank_in = lax.optimization_barrier(jnp.sum(same_owner.astype(jnp.int32), axis=0))

    def per_block(block):
        gradient = (clip_factor * gradients[block].astype(jnp.float32)).astype(jnp.bfloat16)
        current_sketch = sketch[owner_ids[block], slice_ids[block], rank_in[block]]
        return precondition(gradient, current_sketch)
    update, fresh_blocks = lax.map(per_block, block_ids)
    new_sketch = sketch.at[owner_ids, slice_ids, rank_in].set(fresh_blocks)
    return (update, new_sketch)
```

```python
import functools
import math

import jax
import jax.numpy as jnp
from jax import lax
from jax.experimental import pallas as pl
from jax.experimental.pallas import tpu as pltpu
from jax.sharding import PartitionSpec as P

NS_ITERS = 5
DECAY = 0.9
DAMPING = 64.0
FIRST_AXES = (((0,), (0,)), ((), ()))
LAST_AXES = (((1,), (1,)), ((), ()))
MESH = pl.DeviceIdType.MESH
F32 = jnp.float32
BF16 = jnp.bfloat16


def inverse_root(matrix, epsilon):
    identity = jnp.eye(matrix.shape[0], dtype=jnp.float32)
    trace_sum = jnp.trace(matrix) + epsilon
    current = matrix / trace_sum
    inverse = identity
    for repeat in range(NS_ITERS):
        middle = 1.5 * identity - 0.5 * jnp.dot(inverse, current, precision=lax.Precision.HIGHEST)
        current = jnp.dot(current, middle, precision=lax.Precision.HIGHEST)
        inverse = jnp.dot(middle, inverse, precision=lax.Precision.HIGHEST)
    return inverse / jnp.sqrt(trace_sum)


def precondition(gradient, current_sketch):
    identity = jnp.eye(current_sketch.shape[1], dtype=jnp.float32)
    projected = lax.dot_general(
        gradient, current_sketch, FIRST_AXES, preferred_element_type=jnp.float32
    ).astype(jnp.bfloat16)
    gram_matrix = lax.dot_general(
        current_sketch, current_sketch, FIRST_AXES, preferred_element_type=jnp.float32
    ).astype(jnp.bfloat16)
    powered = DECAY * jnp.dot(
        current_sketch, gram_matrix, preferred_element_type=jnp.float32
    ) + jnp.dot(gradient, projected, preferred_element_type=jnp.float32)
    inner_gram = lax.dot_general(powered, powered, FIRST_AXES, precision=lax.Precision.HIGHEST)
    basis_full = jnp.dot(powered, inverse_root(inner_gram, 1e-06), precision=lax.Precision.HIGHEST)
    basis_low = basis_full.astype(jnp.bfloat16)
    coefficients = lax.dot_general(
        gradient, basis_low, FIRST_AXES, preferred_element_type=jnp.float32
    ).astype(jnp.bfloat16)
    alignment = lax.dot_general(
        current_sketch, basis_low, FIRST_AXES, preferred_element_type=jnp.float32
    )
    energy = DECAY * lax.dot_general(
        alignment, alignment, FIRST_AXES, precision=lax.Precision.HIGHEST
    ) + lax.dot_general(coefficients, coefficients, FIRST_AXES, preferred_element_type=jnp.float32)
    root_inverse = inverse_root(energy + DAMPING * identity, 0.0)
    inner_part = jnp.dot(energy, root_inverse, precision=lax.Precision.HIGHEST)
    new_block = jnp.dot(basis_full, inner_part, precision=lax.Precision.HIGHEST).astype(
        jnp.bfloat16
    )
    mix_matrix = math.sqrt(DAMPING) * root_inverse - identity
    side_terms = lax.dot_general(
        coefficients.astype(jnp.float32), mix_matrix, LAST_AXES, precision=lax.Precision.HIGHEST
    ).astype(jnp.bfloat16)
    update_block = (
        gradient.astype(jnp.float32)
        + lax.dot_general(basis_low, side_terms, LAST_AXES, preferred_element_type=jnp.float32)
    ).astype(jnp.bfloat16)
    return (update_block, new_block)


def wait_bytes(ref, sem):
    pltpu.make_async_copy(ref, ref, sem).wait()


def put(src, dst, send, recv, device):
    pltpu.make_async_remote_copy(
        src_ref=src, dst_ref=dst, send_sem=send, recv_sem=recv, device_id=device, device_id_type=MESH
    ).start()


def barrier_with(f, r, nf, nr, with_rep):
    barrier = pltpu.get_barrier_semaphore()

    def to_fsdp(i, carry):
        pl.semaphore_signal(barrier, inc=1, device_id=(lax.rem(f + i, nf), r), device_id_type=MESH)
        return carry

    def to_rep(i, carry):
        pl.semaphore_signal(barrier, inc=1, device_id=(f, lax.rem(r + i, nr)), device_id_type=MESH)
        return carry

    lax.fori_loop(1, nf, to_fsdp, 0)
    if with_rep:
        lax.fori_loop(1, nr, to_rep, 0)
    pl.semaphore_wait(barrier, nf - 1 + (nr - 1 if with_rep else 0))


def gather_kernel(
    nf, nr, slot_ref, part, sk, g_out, z_out, ss_out,
    own, rc, s_a, r_a, s_b, r_b, fin, sk_r, sk_s, ss_a, ss_b,
    own_sem, rc_sem, ra_sem, rb_sem, gz_sem, send_sem,
):
    f = lax.axis_index("fsdp")
    r = lax.axis_index("rep")
    ny = nr // 2
    steps = own.shape[2]
    rows = own.shape[3]
    y = r // 2
    c = lax.rem(r, 2)
    partner = (f, 2 * y + 1 - c)
    ydev = ((f, 2 * lax.rem(y + 1, ny) + c), (f, 2 * lax.rem(y + ny - 1, ny) + c))
    rel = (1, ny - 1)

    for d in (2, 1, 3, 0):
        pltpu.make_async_copy(part.at[2 * lax.rem(y + d, ny) + c], own.at[d], own_sem.at[d]).start()

    barrier_with(f, r, nf, nr, True)

    for k in range(steps):
        for d in (2, 1, 3, 0):
            put(part.at[2 * lax.rem(y + d, ny) + 1 - c, :, k], rc.at[d, :, k], send_sem.at[0], rc_sem.at[d, k], partner)
        if k == 0:
            def spread(i, carry):
                t = lax.rem(f + i, nf)
                put(sk.at[:, pl.ds(pl.multiple_of(t * rows, rows), rows), :], sk_r.at[f], send_sem.at[1], gz_sem.at[0], (t, r))
                return carry

            lax.fori_loop(1, nf, spread, 0)
            mine = pltpu.make_async_copy(sk.at[:, pl.ds(pl.multiple_of(f * rows, rows), rows), :], sk_r.at[f], gz_sem.at[3])
            mine.start()

    for d in (2, 1, 3, 0):
        pltpu.make_async_copy(own.at[d], own.at[d], own_sem.at[d]).wait()

    def both(d, h, k):
        return own[d, h, k].astype(F32) + rc[d, h, k].astype(F32)

    def dependent(k):
        for d in (0, 1):
            wait_bytes(r_a.at[d, k], ra_sem.at[d, k])
            s_b[d, d, k] = (both(rel[d], d, k) + r_a[d, k].astype(F32)).astype(BF16)
            put(s_b.at[d, d, k], r_b.at[d, d, k], send_sem.at[3], rb_sem.at[d, d, k], ydev[d])

    def final(k, total):
        wait_bytes(rc.at[0, :, k], rc_sem.at[0, k])
        for h in (0, 1):
            wait_bytes(r_b.at[1 - h, h, k], rb_sem.at[1 - h, h, k])
            wait_bytes(r_b.at[h, h, k], rb_sem.at[h, h, k])
            value = (both(0, h, k) + (r_b[0, h, k].astype(F32) + r_b[1, h, k].astype(F32))).astype(BF16)
            fin[h, k] = value
            wide = value.astype(F32)
            square = wide * wide
            total = total + jnp.sum(square.reshape(rows // 8, 8, square.shape[1] // 128, 128).transpose(0, 2, 1, 3).reshape(-1, 8, 128), axis=0)
            target = 2 * (h * steps + k) + c

            @pl.when(target != f)
            def _():
                put(fin.at[h, k], g_out.at[f], send_sem.at[4], gz_sem.at[1], (target, r))

            @pl.when(target == f)
            def _():
                g_out[f] = value
        return total

    total = jnp.zeros((8, 128), F32)
    for k in range(steps):
        wait_bytes(rc.at[2, :, k], rc_sem.at[2, k])
        for d in (0, 1):
            s_a[d, k] = both(2, d, k).astype(BF16)
            put(s_a.at[d, k], r_a.at[d, k], send_sem.at[2], ra_sem.at[d, k], ydev[d])
        for d in (0, 1):
            wait_bytes(rc.at[rel[d], :, k], rc_sem.at[rel[d], k])
            s_b[d, 1 - d, k] = both(rel[d], 1 - d, k).astype(BF16)
            put(s_b.at[d, 1 - d, k], r_b.at[d, 1 - d, k], send_sem.at[3], rb_sem.at[d, 1 - d, k], ydev[d])
        if k >= 1:
            dependent(k - 1)
        if k >= 3:
            total = final(k - 3, total)
    dependent(steps - 1)
    for k in range(steps - 3, steps):
        total = final(k, total)

    ss_a[r] = total

    def rep_send(i, carry):
        put(ss_a.at[r], ss_a.at[r], send_sem.at[5], gz_sem.at[4], (f, lax.rem(r + i, nr)))
        return carry

    lax.fori_loop(1, nr, rep_send, 0)

    mine.wait()
    wait_bytes(sk_r.at[pl.ds(0, nf - 1)], gz_sem.at[0])
    for j in range(2 * steps):
        target = 2 * j + c
        slot = slot_ref[j]
        sk_s[j] = sk_r[slot // 2, lax.rem(slot, 2)]

        @pl.when(target != f)
        def _():
            put(sk_s.at[j], z_out.at[f], send_sem.at[6], gz_sem.at[2], (target, r))

        @pl.when(target == f)
        def _():
            z_out[f] = sk_s[j]

    wait_bytes(ss_a.at[pl.ds(0, nr - 1)], gz_sem.at[4])
    ss_b[f] = jnp.sum(ss_a[...], axis=0)

    def fsdp_send(i, carry):
        put(ss_b.at[f], ss_b.at[f], send_sem.at[7], gz_sem.at[5], (lax.rem(f + i, nf), r))
        return carry

    lax.fori_loop(1, nf, fsdp_send, 0)
    wait_bytes(ss_b.at[pl.ds(0, nf - 1)], gz_sem.at[5])
    ss_out[...] = jnp.sum(ss_b[...], axis=0)

    wait_bytes(rc, send_sem.at[0])
    wait_bytes(sk_r.at[pl.ds(0, nf - 1)], send_sem.at[1])
    wait_bytes(s_a, send_sem.at[2])
    wait_bytes(s_b, send_sem.at[3])
    wait_bytes(ss_a.at[pl.ds(0, nr - 1)], send_sem.at[5])
    wait_bytes(ss_b.at[pl.ds(0, nf - 1)], send_sem.at[7])
    busy = (lax.rem(f, 2) == c) & (f < 4 * steps)

    @pl.when(busy)
    def _():
        wait_bytes(g_out.at[pl.ds(0, 2 * steps - 1)], send_sem.at[4])
        wait_bytes(z_out.at[pl.ds(0, 2 * steps - 1)], send_sem.at[6])
        wait_bytes(g_out.at[pl.ds(0, nf - 1)], gz_sem.at[1])
        wait_bytes(z_out.at[pl.ds(0, nf - 1)], gz_sem.at[2])

    @pl.when(jnp.logical_not(busy))
    def _():
        wait_bytes(g_out.at[pl.ds(0, 2 * steps)], send_sem.at[4])
        wait_bytes(z_out.at[pl.ds(0, 2 * steps)], send_sem.at[6])


def scatter_kernel(
    nf, nr, back_ref, up, new, upd_out, nk_out, s_r, s_x, recv_sem, send_sem,
):
    f = lax.axis_index("fsdp")
    r = lax.axis_index("rep")
    c = lax.rem(r, 2)
    blocks = upd_out.shape[0]
    rows = upd_out.shape[1]
    busy = (lax.rem(f, 2) == c) & (f < 2 * blocks)
    j = f // 2
    barrier_with(f, r, nf, nr, False)

    @pl.when(busy)
    def _():
        def send_new(i, carry):
            t = lax.rem(f + i, nf)
            put(new.at[t], s_r.at[j], send_sem.at[0], recv_sem.at[0], (t, r))
            return carry

        def send_up(i, carry):
            t = lax.rem(f + i, nf)
            put(up.at[t], upd_out.at[j], send_sem.at[1], recv_sem.at[1], (t, r))
            return carry

        lax.fori_loop(1, nf, send_new, 0)
        lax.fori_loop(1, nf, send_up, 0)
        s_r[j] = new[f]
        upd_out[j] = up[f]
        wait_bytes(s_r.at[pl.ds(0, blocks - 1)], recv_sem.at[0])

    @pl.when(jnp.logical_not(busy))
    def _():
        wait_bytes(s_r, recv_sem.at[0])

    def spread(i, carry):
        t = lax.rem(f + i, nf)
        for q in (0, 1):
            s_x[t, q] = s_r[back_ref[2 * t + q]]
        put(s_x.at[t], nk_out.at[f], send_sem.at[2], recv_sem.at[2], (t, r))
        return carry

    lax.fori_loop(1, nf, spread, 0)
    for q in (0, 1):
        nk_out[f, q] = s_r[back_ref[2 * f + q]]

    wait_bytes(nk_out.at[pl.ds(0, nf - 1)], recv_sem.at[2])
    wait_bytes(nk_out.at[pl.ds(0, nf - 1)], send_sem.at[2])

    @pl.when(busy)
    def _():
        wait_bytes(upd_out.at[pl.ds(0, blocks - 1)], recv_sem.at[1])
        wait_bytes(new.at[pl.ds(0, nf - 1)], send_sem.at[0])
        wait_bytes(up.at[pl.ds(0, nf - 1)], send_sem.at[1])

    @pl.when(jnp.logical_not(busy))
    def _():
        wait_bytes(upd_out, recv_sem.at[1])


def local(nf, nr, partials, sketch, owner_table):
    blocks_all, rows, width = partials.shape[1:]
    per_slice = blocks_all // nr
    half = per_slice // 2
    rank = sketch.shape[4]
    ny = nr // 2
    vmem = pl.BlockSpec(memory_space=pltpu.VMEM)
    anyw = pl.BlockSpec(memory_space=pl.ANY)
    smem = pl.BlockSpec(memory_space=pltpu.SMEM)
    dma = pltpu.SemaphoreType.DMA

    owners = lax.dynamic_slice_in_dim(owner_table[:, 0], lax.axis_index("rep") * per_slice, per_slice)
    position = jnp.arange(per_slice, dtype=jnp.int32)
    same = (owners[:, None] == owners[None, :]) & (position[:, None] < position[None, :])
    slots = owners * 2 + jnp.sum(same.astype(jnp.int32), axis=0)
    hit = slots[:, None] == jnp.arange(2 * nf, dtype=jnp.int32)[None, :]
    back = jnp.sum(jnp.where(hit, position[:, None], 0), axis=0)
    filled = jnp.sum((owners == lax.axis_index("fsdp")).astype(jnp.int32))

    part = partials.reshape(nr, 2, half, rows, width)
    held = sketch[0, 0]
    g_rows, z_rows, squares = pl.pallas_call(
        functools.partial(gather_kernel, nf, nr),
        out_shape=(
            jax.ShapeDtypeStruct((nf, rows, width), BF16),
            jax.ShapeDtypeStruct((nf, rows, rank), BF16),
            jax.ShapeDtypeStruct((8, 128), F32),
        ),
        in_specs=[smem, anyw, anyw],
        out_specs=(vmem, vmem, vmem),
        scratch_shapes=[
            pltpu.VMEM((ny, 2, half, rows, width), BF16),
            pltpu.VMEM((ny, 2, half, rows, width), BF16),
            pltpu.VMEM((2, half, rows, width), BF16),
            pltpu.VMEM((2, half, rows, width), BF16),
            pltpu.VMEM((2, 2, half, rows, width), BF16),
            pltpu.VMEM((2, 2, half, rows, width), BF16),
            pltpu.VMEM((2, half, rows, width), BF16),
            pltpu.VMEM((nf, 2, rows, rank), BF16),
            pltpu.VMEM((per_slice, rows, rank), BF16),
            pltpu.VMEM((nr, 8, 128), F32),
            pltpu.VMEM((nf, 8, 128), F32),
            dma((ny,)),
            dma((ny, half)),
            dma((2, half)),
            dma((2, 2, half)),
            dma((6,)),
            dma((8,)),
        ],
        compiler_params=pltpu.CompilerParams(collective_id=0, has_side_effects=True),
    )(slots, part, held)

    size = blocks_all * width * width
    sum_squares = jnp.sum(squares)
    clip_factor = jnp.minimum(1.0, 0.5 * math.sqrt(size) / jnp.sqrt(sum_squares + 1e-06))
    gradient = (clip_factor * g_rows.reshape(width, width).astype(F32)).astype(BF16)
    update_block, new_block = precondition(gradient, z_rows.reshape(width, rank))

    upd, fresh = pl.pallas_call(
        functools.partial(scatter_kernel, nf, nr),
        out_shape=(
            jax.ShapeDtypeStruct((per_slice, rows, width), BF16),
            jax.ShapeDtypeStruct((nf, 2, rows, rank), BF16),
        ),
        in_specs=[smem, vmem, vmem],
        out_specs=(vmem, vmem),
        scratch_shapes=[
            pltpu.VMEM((per_slice, rows, rank), BF16),
            pltpu.VMEM((nf, 2, rows, rank), BF16),
            dma((3,)),
            dma((3,)),
        ],
        compiler_params=pltpu.CompilerParams(collective_id=1, has_side_effects=True),
    )(back, update_block.reshape(nf, rows, width), new_block.reshape(nf, rows, rank))
    fresh = fresh.transpose(1, 0, 2, 3).reshape(2, nf * rows, rank)
    keep = jnp.arange(2, dtype=jnp.int32)[:, None, None] < filled
    return upd, jnp.where(keep, fresh, held)[None, None]


def solution(mesh):
    nf, nr = mesh.shape["fsdp"], mesh.shape["rep"]
    return jax.shard_map(
        functools.partial(local, nf, nr),
        mesh=mesh,
        in_specs=(P("rep", None, "fsdp", None), P("fsdp", "rep", None, None, None), P()),
        out_specs=(P("rep", "fsdp", None), P("fsdp", "rep", None, None, None)),
        check_vma=False,
    )
```

```python
import functools
import math

import jax
import jax.numpy as jnp
from jax import lax
from jax.experimental import pallas as pl
from jax.experimental.pallas import tpu as pltpu
from jax.sharding import PartitionSpec as P

NS_ITERS = 5
DECAY = 0.9
DAMPING = 64.0
LAST_AXES = (((1,), (1,)), ((), ()))
MESH = pl.DeviceIdType.MESH
F32 = jnp.float32
BF16 = jnp.bfloat16


def dot(a, b, dims=(((1,), (0,)), ((), ()))):
    return lax.dot_general(a, b, dims, preferred_element_type=F32)


def split(value):
    high = value.astype(BF16)
    return high, (value - high.astype(F32)).astype(BF16)


def inverse_root(matrix, epsilon, eye):
    trace = jnp.sum(jnp.sum(matrix * eye, axis=1, keepdims=True), axis=0, keepdims=True) + epsilon
    state = matrix * (1.0 / trace)
    inverse = 1.5 * eye - 0.5 * state
    for step in range(1, NS_ITERS):
        low = state.astype(BF16)
        half = 1.5 * state - 0.5 * dot(low, low)
        state = 1.5 * half - 0.5 * dot(low, half.astype(BF16))
        low = state.astype(BF16)
        high_part, low_part = split(inverse)
        inverse = 1.5 * inverse - 0.5 * (dot(low, high_part) + dot(low, low_part))
    return inverse * (1.0 / jnp.sqrt(trace))


def wait_bytes(ref, sem):
    pltpu.make_async_copy(ref, ref, sem).wait()


def put(src, dst, send, recv, device):
    pltpu.make_async_remote_copy(
        src_ref=src, dst_ref=dst, send_sem=send, recv_sem=recv, device_id=device, device_id_type=MESH
    ).start()


def barrier_with(f, r, nf, nr, with_rep):
    barrier = pltpu.get_barrier_semaphore()

    def to_fsdp(i, carry):
        pl.semaphore_signal(barrier, inc=1, device_id=(lax.rem(f + i, nf), r), device_id_type=MESH)
        return carry

    def to_rep(i, carry):
        pl.semaphore_signal(barrier, inc=1, device_id=(f, lax.rem(r + i, nr)), device_id_type=MESH)
        return carry

    lax.fori_loop(1, nf, to_fsdp, 0)
    if with_rep:
        lax.fori_loop(1, nr, to_rep, 0)
    pl.semaphore_wait(barrier, nf - 1 + (nr - 1 if with_rep else 0))


def step_kernel(
    nf, nr, limit, table, part, sk, upd_out, nk_out,
    own, rc, s_a, r_a, s_b, r_b, fin, sk_r, sk_s, ss_a, ss_b, g_out, z_out, base, first,
    gs, zt, at, wh, wl, wth, wtl, qb, qt, ht, up, new, s_r, s_x, slots, back,
    own_sem, rc_sem, ra_sem, rb_sem, gz_sem, send_sem, out_sem,
):
    f = lax.axis_index("fsdp")
    r = lax.axis_index("rep")
    ny = nr // 2
    steps = own.shape[2]
    rows = own.shape[3]
    y = r // 2
    c = lax.rem(r, 2)
    partner = (f, 2 * y + 1 - c)
    ydev = ((f, 2 * lax.rem(y + 1, ny) + c), (f, 2 * lax.rem(y + ny - 1, ny) + c))
    rel = (1, ny - 1)

    def place(j):
        n = 2 * j + c
        return n + (n + 4) // 8

    spot = f - (f + 5) // 9
    busy = (lax.rem(f + 5, 9) != 0) & (lax.rem(spot, 2) == c)
    block = spot // 2

    for d in (2, 1, 3, 0):
        pltpu.make_async_copy(part.at[2 * lax.rem(y + d, ny) + c], own.at[d], own_sem.at[d]).start()

    barrier_with(f, r, nf, nr, True)

    def order(i):
        return lax.rem(f + i, steps)

    for i in range(steps):
        k = order(i)
        for d in (2, 1, 3, 0):
            put(part.at[2 * lax.rem(y + d, ny) + 1 - c, :, k], rc.at[d, :, k], send_sem.at[0], rc_sem.at[d, k], partner)
        if i == 0:
            def spread(i, carry):
                t = lax.rem(f + i, nf)
                put(sk.at[:, pl.ds(pl.multiple_of(t * rows, rows), rows), :], sk_r.at[f], send_sem.at[1], gz_sem.at[0], (t, r))
                return carry

            lax.fori_loop(1, nf, spread, 0)
            mine = pltpu.make_async_copy(sk.at[:, pl.ds(pl.multiple_of(f * rows, rows), rows), :], sk_r.at[f], gz_sem.at[3])
            mine.start()

    count = 2 * steps
    owners = [table[r * count + j] for j in range(count)]
    for j in range(count):
        slots[j] = 2 * owners[j] + sum(((owners[i] == owners[j]).astype(jnp.int32) for i in range(j)), jnp.int32(0))

    def invert(t, carry):
        at = jnp.int32(0)
        for j in range(count):
            at = jnp.where(slots[j] == t, j, at)
        back[t] = at
        return carry

    lax.fori_loop(0, 2 * nf, invert, 0)

    for d in (2, 1, 3, 0):
        pltpu.make_async_copy(own.at[d], own.at[d], own_sem.at[d]).wait()

    def both(d, h, k):
        return own[d, h, k].astype(F32) + rc[d, h, k].astype(F32)

    def opposite(k):
        wait_bytes(rc.at[2, :, k], rc_sem.at[2, k])
        for d in (0, 1):
            s_a[d, k] = both(2, d, k).astype(BF16)
            put(s_a.at[d, k], r_a.at[d, k], send_sem.at[2], ra_sem.at[d, k], ydev[d])

    def independent(k):
        for d in (0, 1):
            wait_bytes(rc.at[rel[d], :, k], rc_sem.at[rel[d], k])
            s_b[d, 1 - d, k] = both(rel[d], 1 - d, k).astype(BF16)
            put(s_b.at[d, 1 - d, k], r_b.at[d, 1 - d, k], send_sem.at[3], rb_sem.at[d, 1 - d, k], ydev[d])

    def dependent(k):
        for d in (0, 1):
            wait_bytes(r_a.at[d, k], ra_sem.at[d, k])
            s_b[d, d, k] = (both(rel[d], d, k) + r_a[d, k].astype(F32)).astype(BF16)
            put(s_b.at[d, d, k], r_b.at[d, d, k], send_sem.at[3], rb_sem.at[d, d, k], ydev[d])

    def final(k, total):
        wait_bytes(rc.at[0, :, k], rc_sem.at[0, k])
        for h in (0, 1):
            wait_bytes(r_b.at[1 - h, h, k], rb_sem.at[1 - h, h, k])
            wait_bytes(r_b.at[h, h, k], rb_sem.at[h, h, k])
            value = (both(0, h, k) + (r_b[0, h, k].astype(F32) + r_b[1, h, k].astype(F32))).astype(BF16)
            fin[h, k] = value
            target = place(h * steps + k)

            @pl.when(target != f)
            def _():
                put(fin.at[h, k], g_out.at[f], send_sem.at[4], gz_sem.at[1], (target, r))

            @pl.when(target == f)
            def _():
                g_out[f] = value

            wide = value.astype(F32)
            square = wide * wide
            total = total + jnp.sum(square.reshape(rows // 8, 8, square.shape[1] // 128, 128).transpose(0, 2, 1, 3).reshape(-1, 8, 128), axis=0)
        return total

    def sketches():
        mine.wait()
        wait_bytes(sk_r.at[pl.ds(0, nf - 1)], gz_sem.at[0])
        for i in range(2 * steps):
            j = lax.rem(f + i, 2 * steps)
            target = place(j)
            slot = slots[j]
            sk_s[j] = sk_r[slot // 2, lax.rem(slot, 2)]

            @pl.when(target != f)
            def _():
                put(sk_s.at[j], z_out.at[f], send_sem.at[6], gz_sem.at[2], (target, r))

            @pl.when(target == f)
            def _():
                z_out[f] = sk_s[j]

    total = jnp.zeros((8, 128), F32)
    for i in range(steps + 3):
        if i < steps:
            opposite(order(i))
        if 1 <= i < steps + 1:
            independent(order(i - 1))
        if 2 <= i < steps + 2:
            dependent(order(i - 2))
        if i == steps + 1:
            sketches()
        if i >= 3:
            total = final(order(i - 3), total)

    ss_a[r] = total

    def rep_send(i, carry):
        put(ss_a.at[r], ss_a.at[r], send_sem.at[5], gz_sem.at[4], (f, lax.rem(r + i, nr)))
        return carry

    lax.fori_loop(1, nr, rep_send, 0)
    wait_bytes(ss_a.at[pl.ds(0, nr - 1)], gz_sem.at[4])
    ss_b[f] = jnp.sum(ss_a[...], axis=0)

    def fsdp_send(i, carry):
        put(ss_b.at[f], ss_b.at[f], send_sem.at[7], gz_sem.at[5], (lax.rem(f + i, nf), r))
        return carry

    lax.fori_loop(1, nf, fsdp_send, 0)

    width, rank = g_out.shape[2], z_out.shape[2]

    @pl.when(busy)
    def _():
        wait_bytes(z_out.at[pl.ds(0, nf - 1)], gz_sem.at[2])
        held = z_out[...].reshape(width, rank)
        zt[...] = held.T
        gram = dot(zt[...], held).astype(BF16)
        base[...] = DECAY * dot(held, gram)
        wait_bytes(g_out.at[pl.ds(0, nf - 1)], gz_sem.at[1])
        first[...] = dot(zt[...], g_out[...].reshape(width, width))

    wait_bytes(ss_b.at[pl.ds(0, nf - 1)], gz_sem.at[5])

    @pl.when(busy)
    def _():
        eye = (
            lax.broadcasted_iota(jnp.int32, (rank, rank), 0) == lax.broadcasted_iota(jnp.int32, (rank, rank), 1)
        ).astype(F32)
        held = z_out[...].reshape(width, rank)
        squares = jnp.sum(ss_b[...], axis=0)
        squares = jnp.sum(jnp.sum(squares, axis=1, keepdims=True), axis=0, keepdims=True)
        clip = jnp.minimum(1.0, limit / jnp.sqrt(squares + 1e-06))
        gs[...] = (clip * g_out[...].reshape(width, width).astype(F32)).astype(BF16)
        at[...] = (clip * first[...]).astype(BF16)
        powered = base[...] + dot(gs[...], at[...], LAST_AXES)
        high, low = split(powered)
        wh[...] = high
        wl[...] = low
        wth[...] = high.T
        wtl[...] = low.T
        inner = dot(wth[...], wh[...]) + (dot(wth[...], wl[...]) + dot(wtl[...], wh[...]))
        root_h, root_l = split(inverse_root(inner, 1e-06, eye))
        qb[...] = (dot(wh[...], root_h) + (dot(wh[...], root_l) + dot(wl[...], root_h))).astype(BF16)
        qt[...] = (dot(root_h, wth[...]) + (dot(root_l, wth[...]) + dot(root_h, wtl[...]))).astype(BF16)
        ht[...] = dot(qt[...], gs[...]).astype(BF16)
        align_h, align_l = split(dot(qt[...], held))
        cross = dot(align_h, align_l, LAST_AXES)
        energy = DECAY * (dot(align_h, align_h, LAST_AXES) + (cross + cross.T)) + dot(ht[...], ht[...], LAST_AXES)
        inverse = inverse_root(energy + DAMPING * eye, 0.0, eye)
        energy_h, energy_l = split(energy)
        inverse_h, inverse_l = split(inverse)
        inner_part = dot(energy_h, inverse_h) + (dot(energy_h, inverse_l) + dot(energy_l, inverse_h))
        new[...] = dot(qb[...], inner_part.astype(BF16)).astype(BF16).reshape(nf, rows, rank)

        def send_new(i, carry):
            t = lax.rem(f + i, nf)
            put(new.at[t], s_r.at[block], out_sem.at[0], out_sem.at[1], (t, r))
            return carry

        def send_up(i, carry):
            t = lax.rem(f + i, nf)
            put(up.at[t], upd_out.at[block], out_sem.at[2], out_sem.at[3], (t, r))
            return carry

        lax.fori_loop(1, nf, send_new, 0)
        mix_h, mix_l = split(math.sqrt(DAMPING) * inverse - eye)
        ft = (dot(mix_h, ht[...]) + dot(mix_l, ht[...])).astype(BF16)
        up[...] = (gs[...].astype(F32) + dot(qb[...], ft)).astype(BF16).reshape(nf, rows, width)
        lax.fori_loop(1, nf, send_up, 0)
        s_r[block] = new[f]
        upd_out[block] = up[f]
        wait_bytes(s_r.at[pl.ds(0, count - 1)], out_sem.at[1])

    @pl.when(jnp.logical_not(busy))
    def _():
        wait_bytes(s_r, out_sem.at[1])

    def scatter(i, carry):
        t = lax.rem(f + i, nf)
        for q in (0, 1):
            s_x[t, q] = s_r[back[2 * t + q]]
        put(s_x.at[t], nk_out.at[:, f], out_sem.at[4], out_sem.at[5], (t, r))
        return carry

    lax.fori_loop(1, nf, scatter, 0)
    for q in (0, 1):
        nk_out[q, f] = s_r[back[2 * f + q]]

    wait_bytes(rc, send_sem.at[0])
    wait_bytes(sk_r.at[pl.ds(0, nf - 1)], send_sem.at[1])
    wait_bytes(s_a, send_sem.at[2])
    wait_bytes(s_b, send_sem.at[3])
    wait_bytes(ss_a.at[pl.ds(0, nr - 1)], send_sem.at[5])
    wait_bytes(ss_b.at[pl.ds(0, nf - 1)], send_sem.at[7])
    wait_bytes(s_x.at[pl.ds(0, nf - 1)], out_sem.at[4])
    wait_bytes(nk_out.at[:, pl.ds(0, nf - 1)], out_sem.at[5])

    @pl.when(busy)
    def _():
        wait_bytes(g_out.at[pl.ds(0, count - 1)], send_sem.at[4])
        wait_bytes(z_out.at[pl.ds(0, count - 1)], send_sem.at[6])
        wait_bytes(new.at[pl.ds(0, nf - 1)], out_sem.at[0])
        wait_bytes(up.at[pl.ds(0, nf - 1)], out_sem.at[2])
        wait_bytes(upd_out.at[pl.ds(0, count - 1)], out_sem.at[3])

    @pl.when(jnp.logical_not(busy))
    def _():
        wait_bytes(g_out.at[pl.ds(0, count)], send_sem.at[4])
        wait_bytes(z_out.at[pl.ds(0, count)], send_sem.at[6])
        wait_bytes(upd_out, out_sem.at[3])


def local(nf, nr, partials, sketch, owner_table):
    blocks_all, rows, width = partials.shape[1:]
    per_slice = blocks_all // nr
    half = per_slice // 2
    rank = sketch.shape[4]
    ny = nr // 2
    vmem = pl.BlockSpec(memory_space=pltpu.VMEM)
    anyw = pl.BlockSpec(memory_space=pl.ANY)
    smem = pl.BlockSpec(memory_space=pltpu.SMEM)
    dma = pltpu.SemaphoreType.DMA
    tall, wide = pltpu.VMEM((width, rank), BF16), pltpu.VMEM((rank, width), BF16)
    held = sketch[0, 0]
    upd, fresh = pl.pallas_call(
        functools.partial(step_kernel, nf, nr, 0.5 * math.sqrt(blocks_all * width * width)),
        out_shape=(
            jax.ShapeDtypeStruct((per_slice, rows, width), BF16),
            jax.ShapeDtypeStruct((2, nf, rows, rank), BF16),
        ),
        in_specs=[smem, anyw, anyw],
        out_specs=(vmem, vmem),
        scratch_shapes=[
            pltpu.VMEM((ny, 2, half, rows, width), BF16),
            pltpu.VMEM((ny, 2, half, rows, width), BF16),
            pltpu.VMEM((2, half, rows, width), BF16),
            pltpu.VMEM((2, half, rows, width), BF16),
            pltpu.VMEM((2, 2, half, rows, width), BF16),
            pltpu.VMEM((2, 2, half, rows, width), BF16),
            pltpu.VMEM((2, half, rows, width), BF16),
            pltpu.VMEM((nf, 2, rows, rank), BF16),
            pltpu.VMEM((per_slice, rows, rank), BF16),
            pltpu.VMEM((nr, 8, 128), F32),
            pltpu.VMEM((nf, 8, 128), F32),
            pltpu.VMEM((nf, rows, width), BF16),
            pltpu.VMEM((nf, rows, rank), BF16),
            pltpu.VMEM((width, rank), F32),
            pltpu.VMEM((rank, width), F32),
            pltpu.VMEM((width, width), BF16),
            wide, wide, tall, tall, wide, wide, tall, wide, wide,
            pltpu.VMEM((nf, rows, width), BF16),
            pltpu.VMEM((nf, rows, rank), BF16),
            pltpu.VMEM((per_slice, rows, rank), BF16),
            pltpu.VMEM((nf, 2, rows, rank), BF16),
            pltpu.SMEM((per_slice,), jnp.int32),
            pltpu.SMEM((2 * nf,), jnp.int32),
            dma((ny,)),
            dma((ny, half)),
            dma((2, half)),
            dma((2, 2, half)),
            dma((6,)),
            dma((8,)),
            dma((6,)),
        ],
        compiler_params=pltpu.CompilerParams(collective_id=0, has_side_effects=True),
    )(owner_table[:, 0], partials.reshape(nr, 2, half, rows, width), held)

    owners = lax.dynamic_slice_in_dim(owner_table[:, 0], lax.axis_index("rep") * per_slice, per_slice)
    filled = jnp.sum((owners == lax.axis_index("fsdp")).astype(jnp.int32))
    keep = jnp.arange(2, dtype=jnp.int32)[:, None, None] < filled
    return upd, jnp.where(keep, fresh.reshape(2, width, rank), held)[None, None]


def solution(mesh):
    nf, nr = mesh.shape["fsdp"], mesh.shape["rep"]
    return jax.shard_map(
        functools.partial(local, nf, nr),
        mesh=mesh,
        in_specs=(P("rep", None, "fsdp", None), P("fsdp", "rep", None, None, None), P()),
        out_specs=(P("rep", "fsdp", None), P("fsdp", "rep", None, None, None)),
        check_vma=False,
    )
```

```python
import functools
import math

import jax
import jax.numpy as jnp
from jax import lax
from jax.experimental import pallas as pl
from jax.experimental.pallas import tpu as pltpu
from jax.sharding import PartitionSpec as P

NS_ITERS = 5
DECAY = 0.9
DAMPING = 64.0
LAST_AXES = (((1,), (1,)), ((), ()))
MESH = pl.DeviceIdType.MESH
F32 = jnp.float32
BF16 = jnp.bfloat16


def dot(a, b, dims=(((1,), (0,)), ((), ()))):
    return lax.dot_general(a, b, dims, preferred_element_type=F32)


def split(value):
    high = value.astype(BF16)
    return high, (value - high.astype(F32)).astype(BF16)


def inverse_root(matrix, epsilon, eye):
    trace = jnp.sum(jnp.sum(matrix * eye, axis=1, keepdims=True), axis=0, keepdims=True) + epsilon
    state = matrix * (1.0 / trace)
    inverse = 1.5 * eye - 0.5 * state
    for step in range(1, NS_ITERS):
        low = state.astype(BF16)
        half = 1.5 * state - 0.5 * dot(low, low)
        state = 1.5 * half - 0.5 * dot(low, half.astype(BF16))
        low = state.astype(BF16)
        high_part, low_part = split(inverse)
        inverse = 1.5 * inverse - 0.5 * (dot(low, high_part) + dot(low, low_part))
    return inverse * (1.0 / jnp.sqrt(trace))


def wait_bytes(ref, sem):
    pltpu.make_async_copy(ref, ref, sem).wait()


def put(src, dst, send, recv, device):
    pltpu.make_async_remote_copy(
        src_ref=src, dst_ref=dst, send_sem=send, recv_sem=recv, device_id=device, device_id_type=MESH
    ).start()


def barrier_with(f, r, nf, nr, with_rep):
    barrier = pltpu.get_barrier_semaphore()

    def to_fsdp(i, carry):
        pl.semaphore_signal(barrier, inc=1, device_id=(lax.rem(f + i, nf), r), device_id_type=MESH)
        return carry

    def to_rep(i, carry):
        pl.semaphore_signal(barrier, inc=1, device_id=(f, lax.rem(r + i, nr)), device_id_type=MESH)
        return carry

    lax.fori_loop(1, nf, to_fsdp, 0)
    if with_rep:
        lax.fori_loop(1, nr, to_rep, 0)
    pl.semaphore_wait(barrier, nf - 1 + (nr - 1 if with_rep else 0))


def step_kernel(
    nf, nr, limit, table, part, sk, upd_out, nk_out,
    own, rc, s_a, r_a, s_b, r_b, fin, sk_r, sk_s, ss_a, ss_b, g_out, z_out, z_in, base, first,
    gs, zt, at, wh, wl, wth, wtl, qb, qt, ht, up, new, s_r, s_x, slots, back,
    own_sem, rc_sem, ra_sem, rb_sem, gz_sem, send_sem, out_sem,
):
    f = lax.axis_index("fsdp")
    r = lax.axis_index("rep")
    ny = nr // 2
    steps = own.shape[2]
    rows = own.shape[3]
    y = r // 2
    c = lax.rem(r, 2)
    z_one = z_out.reshape(z_out.shape[0] * z_out.shape[1], *z_out.shape[2:])
    nx, nz, npiece = 4, nf // 4, nf // 2
    prow = sk_r.shape[2]
    z, x = f // nx, lax.rem(f, nx)
    partner = (f, 2 * y + 1 - c)
    ydev = ((f, 2 * lax.rem(y + 1, ny) + c), (f, 2 * lax.rem(y + ny - 1, ny) + c))
    rel = (1, ny - 1)

    def place(j):
        n = 2 * j + c
        return n + (n + 4) // 8

    spot = f - (f + 5) // 9
    busy = (lax.rem(f + 5, 9) != 0) & (lax.rem(spot, 2) == c)
    block = spot // 2

    for d in (2, 1, 3, 0):
        pltpu.make_async_copy(part.at[2 * lax.rem(y + d, ny) + c], own.at[d], own_sem.at[d]).start()

    barrier_with(f, r, nf, nr, True)

    def order(i):
        return lax.rem(f + i, steps)

    for i in range(steps):
        k = order(i)
        for d in (2, 1, 3, 0):
            put(part.at[2 * lax.rem(y + d, ny) + 1 - c, :, k], rc.at[d, :, k], send_sem.at[0], rc_sem.at[d, k], partner)

    def away(level):
        return jnp.where(lax.rem(level, 2) == 0, 2, nz - 2)

    def near(i, two):
        level = lax.rem(z + jnp.where(i // nx == 3, two, (0, 1, nz - 1, 0)[i // nx]), nz)
        return level, level * nx + lax.rem(x + i % nx, nx)

    def piece_of(t):
        return lax.rem(t, npiece)

    def cut(t):
        return pl.ds(pl.multiple_of(piece_of(t) * prow, prow), prow)

    mine = pltpu.make_async_copy(sk.at[:, cut(f), :], sk_r.at[f], gz_sem.at[3])
    mine.start()
    for i in range(npiece - 1, 0, -1):
        level, t = near(i, nz - away(z))
        put(sk.at[:, cut(t), :], sk_r.at[f], send_sem.at[1], gz_sem.at[0], (t, r))

    count = 2 * steps
    owners = [table[r * count + j] for j in range(count)]
    for j in range(count):
        slots[j] = 2 * owners[j] + sum(((owners[i] == owners[j]).astype(jnp.int32) for i in range(j)), jnp.int32(0))

    def invert(t, carry):
        at = jnp.int32(0)
        for j in range(count):
            at = jnp.where(slots[j] == t, j, at)
        back[t] = at
        return carry

    lax.fori_loop(0, 2 * nf, invert, 0)

    for d in (2, 1, 3, 0):
        pltpu.make_async_copy(own.at[d], own.at[d], own_sem.at[d]).wait()

    def both(d, h, k):
        return own[d, h, k].astype(F32) + rc[d, h, k].astype(F32)

    def opposite(k):
        wait_bytes(rc.at[2, :, k], rc_sem.at[2, k])
        for d in (0, 1):
            s_a[d, k] = both(2, d, k).astype(BF16)
            put(s_a.at[d, k], r_a.at[d, k], send_sem.at[2], ra_sem.at[d, k], ydev[d])

    def independent(k):
        for d in (0, 1):
            wait_bytes(rc.at[rel[d], :, k], rc_sem.at[rel[d], k])
            s_b[d, 1 - d, k] = both(rel[d], 1 - d, k).astype(BF16)
            put(s_b.at[d, 1 - d, k], r_b.at[d, 1 - d, k], send_sem.at[3], rb_sem.at[d, 1 - d, k], ydev[d])

    def dependent(k):
        for d in (0, 1):
            wait_bytes(r_a.at[d, k], ra_sem.at[d, k])
            s_b[d, d, k] = (both(rel[d], d, k) + r_a[d, k].astype(F32)).astype(BF16)
            put(s_b.at[d, d, k], r_b.at[d, d, k], send_sem.at[3], rb_sem.at[d, d, k], ydev[d])

    def final(k, total):
        wait_bytes(rc.at[0, :, k], rc_sem.at[0, k])
        for h in (0, 1):
            wait_bytes(r_b.at[1 - h, h, k], rb_sem.at[1 - h, h, k])
            wait_bytes(r_b.at[h, h, k], rb_sem.at[h, h, k])
            value = (both(0, h, k) + (r_b[0, h, k].astype(F32) + r_b[1, h, k].astype(F32))).astype(BF16)
            fin[h, k] = value
            target = place(h * steps + k)

            @pl.when(target != f)
            def _():
                put(fin.at[h, k], g_out.at[f], send_sem.at[4], gz_sem.at[1], (target, r))

            @pl.when(target == f)
            def _():
                g_out[f] = value

            wide = value.astype(F32)
            square = wide * wide
            total = total + jnp.sum(square.reshape(rows // 8, 8, square.shape[1] // 128, 128).transpose(0, 2, 1, 3).reshape(-1, 8, 128), axis=0)
        return total

    def sketches():
        mine.wait()
        wait_bytes(sk_r.at[pl.ds(0, npiece - 1)], gz_sem.at[0])
        for i in range(2 * steps):
            j = lax.rem(f + i, 2 * steps)
            target = place(j)
            slot = slots[j]
            owner = slot // 2
            apart = lax.rem(owner // nx - z + nz, nz)
            here = (apart <= 1) | (apart == nz - 1) | (apart == away(z))
            sk_s[j] = sk_r[jnp.where(here, owner, f), lax.rem(slot, 2)]

            @pl.when(target != f)
            def _():
                put(sk_s.at[j], z_out.at[f // npiece, piece_of(f)], send_sem.at[6], gz_sem.at[2], (target, r))

            @pl.when(target == f)
            def _():
                z_out[f // npiece, piece_of(f)] = sk_s[j]

    total = jnp.zeros((8, 128), F32)
    for i in range(steps + 3):
        if i < steps:
            opposite(order(i))
        if 1 <= i < steps + 1:
            independent(order(i - 1))
        if 2 <= i < steps + 2:
            dependent(order(i - 2))
        if i == steps + 1:
            sketches()
        if i >= 3:
            total = final(order(i - 3), total)

    ss_a[r] = total

    def rep_send(i, carry):
        put(ss_a.at[r], ss_a.at[r], send_sem.at[5], gz_sem.at[4], (f, lax.rem(r + i, nr)))
        return carry

    lax.fori_loop(1, nr, rep_send, 0)
    wait_bytes(ss_a.at[pl.ds(0, nr - 1)], gz_sem.at[4])
    ss_b[f] = jnp.sum(ss_a[...], axis=0)

    def fsdp_send(i, carry):
        put(ss_b.at[f], ss_b.at[f], send_sem.at[7], gz_sem.at[5], (lax.rem(f + i, nf), r))
        return carry

    lax.fori_loop(1, nf, fsdp_send, 0)

    width, rank = g_out.shape[2], sk_r.shape[3]

    @pl.when(busy)
    def _():
        wait_bytes(z_one.at[pl.ds(0, nf - 1)], gz_sem.at[2])
        level = slots[block] // (2 * nx)
        for k in range(nz // 2):
            apart = lax.rem(k - level + nz, nz)
            low = (apart <= 1) | (apart == nz - 1) | (apart == nz - away(level))
            z_in[k * nx : (k + 1) * nx] = z_out[jnp.where(low, 0, 1), k * nx : (k + 1) * nx]
        held = z_in[...].reshape(width, rank)
        zt[...] = held.T
        gram = dot(zt[...], held).astype(BF16)
        base[...] = DECAY * dot(held, gram)
        wait_bytes(g_out.at[pl.ds(0, nf - 1)], gz_sem.at[1])
        first[...] = dot(zt[...], g_out[...].reshape(width, width))

    wait_bytes(ss_b.at[pl.ds(0, nf - 1)], gz_sem.at[5])

    @pl.when(busy)
    def _():
        eye = (
            lax.broadcasted_iota(jnp.int32, (rank, rank), 0) == lax.broadcasted_iota(jnp.int32, (rank, rank), 1)
        ).astype(F32)
        held = z_in[...].reshape(width, rank)
        squares = jnp.sum(ss_b[...], axis=0)
        squares = jnp.sum(jnp.sum(squares, axis=1, keepdims=True), axis=0, keepdims=True)
        clip = jnp.minimum(1.0, limit / jnp.sqrt(squares + 1e-06))
        gs[...] = (clip * g_out[...].reshape(width, width).astype(F32)).astype(BF16)
        at[...] = (clip * first[...]).astype(BF16)
        powered = base[...] + dot(gs[...], at[...], LAST_AXES)
        high, low = split(powered)
        wh[...] = high
        wl[...] = low
        wth[...] = high.T
        wtl[...] = low.T
        inner = dot(wth[...], wh[...]) + (dot(wth[...], wl[...]) + dot(wtl[...], wh[...]))
        root_h, root_l = split(inverse_root(inner, 1e-06, eye))
        qb[...] = (dot(wh[...], root_h) + (dot(wh[...], root_l) + dot(wl[...], root_h))).astype(BF16)
        qt[...] = (dot(root_h, wth[...]) + (dot(root_l, wth[...]) + dot(root_h, wtl[...]))).astype(BF16)
        ht[...] = dot(qt[...], gs[...]).astype(BF16)
        align_h, align_l = split(dot(qt[...], held))
        cross = dot(align_h, align_l, LAST_AXES)
        energy = DECAY * (dot(align_h, align_h, LAST_AXES) + (cross + cross.T)) + dot(ht[...], ht[...], LAST_AXES)
        inverse = inverse_root(energy + DAMPING * eye, 0.0, eye)
        energy_h, energy_l = split(energy)
        inverse_h, inverse_l = split(inverse)
        inner_part = dot(energy_h, inverse_h) + (dot(energy_h, inverse_l) + dot(energy_l, inverse_h))
        new[...] = dot(qb[...], inner_part.astype(BF16)).astype(BF16).reshape(npiece, prow, rank)

        def send_new(i, carry):
            t = lax.rem(f + i, nf)
            put(new.at[piece_of(t)], s_r.at[block], out_sem.at[0], out_sem.at[1], (t, r))
            return carry

        def send_up(i, carry):
            t = lax.rem(f + i, nf)
            put(up.at[t], upd_out.at[block], out_sem.at[2], out_sem.at[3], (t, r))
            return carry

        lax.fori_loop(1, nf, send_new, 0)
        mix_h, mix_l = split(math.sqrt(DAMPING) * inverse - eye)
        ft = (dot(mix_h, ht[...]) + dot(mix_l, ht[...])).astype(BF16)
        up[...] = (gs[...].astype(F32) + dot(qb[...], ft)).astype(BF16).reshape(nf, rows, width)
        lax.fori_loop(1, nf, send_up, 0)
        s_r[block] = new[piece_of(f)]
        upd_out[block] = up[f]
        wait_bytes(s_r.at[pl.ds(0, count - 1)], out_sem.at[1])

    @pl.when(jnp.logical_not(busy))
    def _():
        wait_bytes(s_r, out_sem.at[1])

    for i in range(npiece - 1, 0, -1):
        level, t = near(i, away(z))
        for q in (0, 1):
            s_x[i, q] = s_r[back[2 * t + q]]
        put(s_x.at[i], nk_out.at[:, piece_of(f)], out_sem.at[4], out_sem.at[5], (t, r))
    for q in (0, 1):
        nk_out[q, piece_of(f)] = s_r[back[2 * f + q]]

    wait_bytes(rc, send_sem.at[0])
    wait_bytes(sk_r.at[pl.ds(0, npiece - 1)], send_sem.at[1])
    wait_bytes(s_a, send_sem.at[2])
    wait_bytes(s_b, send_sem.at[3])
    wait_bytes(ss_a.at[pl.ds(0, nr - 1)], send_sem.at[5])
    wait_bytes(ss_b.at[pl.ds(0, nf - 1)], send_sem.at[7])
    wait_bytes(s_x.at[pl.ds(0, npiece - 1)], out_sem.at[4])
    wait_bytes(nk_out.at[:, pl.ds(0, npiece - 1)], out_sem.at[5])

    @pl.when(busy)
    def _():
        wait_bytes(g_out.at[pl.ds(0, count - 1)], send_sem.at[4])
        wait_bytes(z_one.at[pl.ds(0, count - 1)], send_sem.at[6])
        wait_bytes(z_one.at[pl.ds(0, nf - 1)], out_sem.at[0])
        wait_bytes(up.at[pl.ds(0, nf - 1)], out_sem.at[2])
        wait_bytes(upd_out.at[pl.ds(0, count - 1)], out_sem.at[3])

    @pl.when(jnp.logical_not(busy))
    def _():
        wait_bytes(g_out.at[pl.ds(0, count)], send_sem.at[4])
        wait_bytes(z_one.at[pl.ds(0, count)], send_sem.at[6])
        wait_bytes(upd_out, out_sem.at[3])


def finish_kernel(count, table, upd, fresh, held, upd_out, sketch_out, sem):
    first = pltpu.make_async_copy(upd, upd_out, sem.at[0])
    first.start()
    f = lax.axis_index("fsdp")
    base = lax.axis_index("rep") * count
    filled = sum(((table[base + j] == f).astype(jnp.int32) for j in range(count)), jnp.int32(0))
    for q in (0, 1):

        @pl.when(q < filled)
        def _():
            pltpu.make_async_copy(fresh.at[q], sketch_out.at[0, 0, q], sem.at[1 + q]).start()

        @pl.when(q >= filled)
        def _():
            pltpu.make_async_copy(held.at[q], sketch_out.at[0, 0, q], sem.at[1 + q]).start()

    first.wait()
    for q in (0, 1):
        pltpu.make_async_copy(fresh.at[q], sketch_out.at[0, 0, q], sem.at[1 + q]).wait()


def local(nf, nr, partials, sketch, owner_table):
    blocks_all, rows, width = partials.shape[1:]
    per_slice = blocks_all // nr
    half = per_slice // 2
    rank = sketch.shape[4]
    ny = nr // 2
    vmem = pl.BlockSpec(memory_space=pltpu.VMEM)
    anyw = pl.BlockSpec(memory_space=pl.ANY)
    smem = pl.BlockSpec(memory_space=pltpu.SMEM)
    dma = pltpu.SemaphoreType.DMA
    tall, wide = pltpu.VMEM((width, rank), BF16), pltpu.VMEM((rank, width), BF16)
    held = sketch[0, 0]
    table = owner_table[:, 0]
    upd, fresh = pl.pallas_call(
        functools.partial(step_kernel, nf, nr, 0.5 * math.sqrt(blocks_all * width * width)),
        out_shape=(
            jax.ShapeDtypeStruct((per_slice, rows, width), BF16),
            jax.ShapeDtypeStruct((2, nf // 2, 2 * rows, rank), BF16),
        ),
        in_specs=[smem, anyw, anyw],
        out_specs=(vmem, vmem),
        scratch_shapes=[
            pltpu.VMEM((ny, 2, half, rows, width), BF16),
            pltpu.VMEM((ny, 2, half, rows, width), BF16),
            pltpu.VMEM((2, half, rows, width), BF16),
            pltpu.VMEM((2, half, rows, width), BF16),
            pltpu.VMEM((2, 2, half, rows, width), BF16),
            pltpu.VMEM((2, 2, half, rows, width), BF16),
            pltpu.VMEM((2, half, rows, width), BF16),
            pltpu.VMEM((nf, 2, 2 * rows, rank), BF16),
            pltpu.VMEM((per_slice, 2 * rows, rank), BF16),
            pltpu.VMEM((nr, 8, 128), F32),
            pltpu.VMEM((nf, 8, 128), F32),
            pltpu.VMEM((nf, rows, width), BF16),
            pltpu.VMEM((2, nf // 2, 2 * rows, rank), BF16),
            pltpu.VMEM((nf // 2, 2 * rows, rank), BF16),
            pltpu.VMEM((width, rank), F32),
            pltpu.VMEM((rank, width), F32),
            pltpu.VMEM((width, width), BF16),
            wide, wide, tall, tall, wide, wide, tall, wide, wide,
            pltpu.VMEM((nf, rows, width), BF16),
            pltpu.VMEM((nf // 2, 2 * rows, rank), BF16),
            pltpu.VMEM((per_slice, 2 * rows, rank), BF16),
            pltpu.VMEM((nf // 2, 2, 2 * rows, rank), BF16),
            pltpu.SMEM((per_slice,), jnp.int32),
            pltpu.SMEM((2 * nf,), jnp.int32),
            dma((ny,)),
            dma((ny, half)),
            dma((2, half)),
            dma((2, 2, half)),
            dma((6,)),
            dma((8,)),
            dma((6,)),
        ],
        compiler_params=pltpu.CompilerParams(collective_id=0, has_side_effects=True, vmem_limit_bytes=48 * 2**20),
    )(table, partials.reshape(nr, 2, half, rows, width), held)

    return pl.pallas_call(
        functools.partial(finish_kernel, per_slice),
        out_shape=(
            jax.ShapeDtypeStruct((per_slice, rows, width), BF16),
            jax.ShapeDtypeStruct((1, 1, 2, width, rank), BF16),
        ),
        in_specs=[smem, vmem, vmem, vmem],
        out_specs=(anyw, anyw),
        scratch_shapes=[dma((3,))],
        compiler_params=pltpu.CompilerParams(vmem_limit_bytes=4 * 2**20),
    )(table, upd, fresh.reshape(2, width, rank), held)


def solution(mesh):
    nf, nr = mesh.shape["fsdp"], mesh.shape["rep"]
    return jax.shard_map(
        functools.partial(local, nf, nr),
        mesh=mesh,
        in_specs=(P("rep", None, "fsdp", None), P("fsdp", "rep", None, None, None), P()),
        out_specs=(P("rep", "fsdp", None), P("fsdp", "rep", None, None, None)),
        check_vma=False,
    )
```

```python
import functools
import math

import jax
import jax.numpy as jnp
from jax import lax
from jax.experimental import pallas as pl
from jax.experimental.pallas import tpu as pltpu
from jax.sharding import PartitionSpec as P

NS_ITERS = 5
DECAY = 0.9
DAMPING = 64.0
LAST_AXES = (((1,), (1,)), ((), ()))
MESH = pl.DeviceIdType.MESH
F32 = jnp.float32
BF16 = jnp.bfloat16


def dot(a, b, dims=(((1,), (0,)), ((), ()))):
    return lax.dot_general(a, b, dims, preferred_element_type=F32)


def split(value):
    high = value.astype(BF16)
    return high, (value - high.astype(F32)).astype(BF16)


def inverse_root(matrix, epsilon, eye):
    trace = jnp.sum(jnp.sum(matrix * eye, axis=1, keepdims=True), axis=0, keepdims=True) + epsilon
    state = matrix * (1.0 / trace)
    inverse = 1.5 * eye - 0.5 * state
    for step in range(1, NS_ITERS):
        low = state.astype(BF16)
        half = 1.5 * state - 0.5 * dot(low, low)
        state = 1.5 * half - 0.5 * dot(low, half.astype(BF16))
        low = state.astype(BF16)
        high_part, low_part = split(inverse)
        inverse = 1.5 * inverse - 0.5 * (dot(low, high_part) + dot(low, low_part))
    return inverse * (1.0 / jnp.sqrt(trace))


def wait_bytes(ref, sem):
    pltpu.make_async_copy(ref, ref, sem).wait()


def put(src, dst, send, recv, device):
    pltpu.make_async_remote_copy(
        src_ref=src, dst_ref=dst, send_sem=send, recv_sem=recv, device_id=device, device_id_type=MESH
    ).start()


def barrier_with(f, r, nf, nr, with_rep):
    barrier = pltpu.get_barrier_semaphore()

    def to_fsdp(i, carry):
        pl.semaphore_signal(barrier, inc=1, device_id=(lax.rem(f + i, nf), r), device_id_type=MESH)
        return carry

    def to_rep(i, carry):
        pl.semaphore_signal(barrier, inc=1, device_id=(f, lax.rem(r + i, nr)), device_id_type=MESH)
        return carry

    lax.fori_loop(1, nf, to_fsdp, 0)
    if with_rep:
        lax.fori_loop(1, nr, to_rep, 0)
    pl.semaphore_wait(barrier, nf - 1 + (nr - 1 if with_rep else 0))


def step_kernel(
    nf, nr, limit, table_in, part, sk, upd_out, nk_out,
    own, rc, s_a, r_a, s_b, r_b, fin, sk_r, sk_s, ss_a, ss_b, g_out, z_out, z_in, base, first,
    gs, zt, at, wh, wl, wth, wtl, qb, qt, ht, up, new, s_r, s_x, slots, back, table,
    tab_sem, own_sem, rc_sem, ra_sem, rb_sem, gz_sem, send_sem, out_sem,
):
    f = lax.axis_index("fsdp")
    r = lax.axis_index("rep")
    ny = nr // 2
    steps = own.shape[2]
    rows = own.shape[3]
    y = r // 2
    c = lax.rem(r, 2)
    z_one = z_out.reshape(z_out.shape[0] * z_out.shape[1], *z_out.shape[2:])
    nx, nz, npiece = 4, nf // 4, nf // 2
    prow = sk_r.shape[2]
    z, x = f // nx, lax.rem(f, nx)
    partner = (f, 2 * y + 1 - c)
    ydev = ((f, 2 * lax.rem(y + 1, ny) + c), (f, 2 * lax.rem(y + ny - 1, ny) + c))
    rel = (1, ny - 1)

    def place(j):
        n = 2 * j + c
        return n + (n + 4) // 8

    spot = f - (f + 5) // 9
    busy = (lax.rem(f + 5, 9) != 0) & (lax.rem(spot, 2) == c)
    block = spot // 2

    owners_in = pltpu.make_async_copy(table_in, table, tab_sem.at[0])
    owners_in.start()

    for d in (2, 1, 3, 0):
        pltpu.make_async_copy(part.at[2 * lax.rem(y + d, ny) + c], own.at[d], own_sem.at[d]).start()

    barrier_with(f, r, nf, nr, True)

    def order(i):
        return lax.rem(f + i, steps)

    for i in range(steps):
        k = order(i)
        for d in (2, 1, 3, 0):
            put(part.at[2 * lax.rem(y + d, ny) + 1 - c, :, k], rc.at[d, :, k], send_sem.at[0], rc_sem.at[d, k], partner)

    def away(level):
        return jnp.where(lax.rem(level, 2) == 0, 2, nz - 2)

    def near(i, two):
        level = lax.rem(z + jnp.where(i // nx == 3, two, (0, 1, nz - 1, 0)[i // nx]), nz)
        return level, level * nx + lax.rem(x + i % nx, nx)

    def piece_of(t):
        return lax.rem(t, npiece)

    def cut(t):
        return pl.ds(pl.multiple_of(piece_of(t) * prow, prow), prow)

    mine = pltpu.make_async_copy(sk.at[:, cut(f), :], sk_r.at[f], gz_sem.at[3])
    mine.start()
    for i in range(npiece - 1, 0, -1):
        level, t = near(i, nz - away(z))
        put(sk.at[:, cut(t), :], sk_r.at[f], send_sem.at[1], gz_sem.at[0], (t, r))

    count = 2 * steps
    owners_in.wait()
    owners = [table[r * count + j] for j in range(count)]
    for j in range(count):
        slots[j] = 2 * owners[j] + sum(((owners[i] == owners[j]).astype(jnp.int32) for i in range(j)), jnp.int32(0))

    def invert(t, carry):
        at = jnp.int32(0)
        for j in range(count):
            at = jnp.where(slots[j] == t, j, at)
        back[t] = at
        return carry

    lax.fori_loop(0, 2 * nf, invert, 0)

    for d in (2, 1, 3, 0):
        pltpu.make_async_copy(own.at[d], own.at[d], own_sem.at[d]).wait()

    def both(d, h, k):
        return own[d, h, k].astype(F32) + rc[d, h, k].astype(F32)

    def opposite(k):
        wait_bytes(rc.at[2, :, k], rc_sem.at[2, k])
        for d in (0, 1):
            s_a[d, k] = both(2, d, k).astype(BF16)
            put(s_a.at[d, k], r_a.at[d, k], send_sem.at[2], ra_sem.at[d, k], ydev[d])

    def independent(k):
        for d in (0, 1):
            wait_bytes(rc.at[rel[d], :, k], rc_sem.at[rel[d], k])
            s_b[d, 1 - d, k] = both(rel[d], 1 - d, k).astype(BF16)
            put(s_b.at[d, 1 - d, k], r_b.at[d, 1 - d, k], send_sem.at[3], rb_sem.at[d, 1 - d, k], ydev[d])

    def dependent(k):
        for d in (0, 1):
            wait_bytes(r_a.at[d, k], ra_sem.at[d, k])
            s_b[d, d, k] = (both(rel[d], d, k) + r_a[d, k].astype(F32)).astype(BF16)
            put(s_b.at[d, d, k], r_b.at[d, d, k], send_sem.at[3], rb_sem.at[d, d, k], ydev[d])

    def final(k, total):
        wait_bytes(rc.at[0, :, k], rc_sem.at[0, k])
        for h in (0, 1):
            wait_bytes(r_b.at[1 - h, h, k], rb_sem.at[1 - h, h, k])
            wait_bytes(r_b.at[h, h, k], rb_sem.at[h, h, k])
            value = (both(0, h, k) + (r_b[0, h, k].astype(F32) + r_b[1, h, k].astype(F32))).astype(BF16)
            fin[h, k] = value
            target = place(h * steps + k)

            @pl.when(target != f)
            def _():
                put(fin.at[h, k], g_out.at[f], send_sem.at[4], gz_sem.at[1], (target, r))

            @pl.when(target == f)
            def _():
                g_out[f] = value

            wide = value.astype(F32)
            square = wide * wide
            total = total + jnp.sum(square.reshape(rows // 8, 8, square.shape[1] // 128, 128).transpose(0, 2, 1, 3).reshape(-1, 8, 128), axis=0)
        return total

    def sketches():
        mine.wait()
        wait_bytes(sk_r.at[pl.ds(0, npiece - 1)], gz_sem.at[0])
        for i in range(2 * steps):
            j = lax.rem(f + i, 2 * steps)
            target = place(j)
            slot = slots[j]
            owner = slot // 2
            apart = lax.rem(owner // nx - z + nz, nz)
            here = (apart <= 1) | (apart == nz - 1) | (apart == away(z))
            sk_s[j] = sk_r[jnp.where(here, owner, f), lax.rem(slot, 2)]

            @pl.when(target != f)
            def _():
                put(sk_s.at[j], z_out.at[f // npiece, piece_of(f)], send_sem.at[6], gz_sem.at[2], (target, r))

            @pl.when(target == f)
            def _():
                z_out[f // npiece, piece_of(f)] = sk_s[j]

    total = jnp.zeros((8, 128), F32)
    for i in range(steps + 3):
        if i < steps:
            opposite(order(i))
        if 1 <= i < steps + 1:
            independent(order(i - 1))
        if 2 <= i < steps + 2:
            dependent(order(i - 2))
        if i == 4:
            sketches()
        if i >= 3:
            total = final(order(i - 3), total)

    ss_a[r] = total

    def rep_send(i, carry):
        put(ss_a.at[r], ss_a.at[r], send_sem.at[5], gz_sem.at[4], (f, lax.rem(r + i, nr)))
        return carry

    lax.fori_loop(1, nr, rep_send, 0)
    wait_bytes(ss_a.at[pl.ds(0, nr - 1)], gz_sem.at[4])
    ss_b[f] = jnp.sum(ss_a[...], axis=0)

    def fsdp_send(i, carry):
        put(ss_b.at[f], ss_b.at[f], send_sem.at[7], gz_sem.at[5], (lax.rem(f + i, nf), r))
        return carry

    lax.fori_loop(1, nf, fsdp_send, 0)

    width, rank = g_out.shape[2], sk_r.shape[3]

    @pl.when(busy)
    def _():
        wait_bytes(z_one.at[pl.ds(0, nf - 1)], gz_sem.at[2])
        level = slots[block] // (2 * nx)
        for k in range(nz // 2):
            apart = lax.rem(k - level + nz, nz)
            low = (apart <= 1) | (apart == nz - 1) | (apart == nz - away(level))
            z_in[k * nx : (k + 1) * nx] = z_out[jnp.where(low, 0, 1), k * nx : (k + 1) * nx]
        held = z_in[...].reshape(width, rank)
        zt[...] = held.T
        gram = dot(zt[...], held).astype(BF16)
        base[...] = DECAY * dot(held, gram)
        wait_bytes(g_out.at[pl.ds(0, nf - 1)], gz_sem.at[1])
        first[...] = dot(zt[...], g_out[...].reshape(width, width))

    wait_bytes(ss_b.at[pl.ds(0, nf - 1)], gz_sem.at[5])

    @pl.when(busy)
    def _():
        eye = (
            lax.broadcasted_iota(jnp.int32, (rank, rank), 0) == lax.broadcasted_iota(jnp.int32, (rank, rank), 1)
        ).astype(F32)
        held = z_in[...].reshape(width, rank)
        squares = jnp.sum(ss_b[...], axis=0)
        squares = jnp.sum(jnp.sum(squares, axis=1, keepdims=True), axis=0, keepdims=True)
        clip = jnp.minimum(1.0, limit / jnp.sqrt(squares + 1e-06))
        gs[...] = (clip * g_out[...].reshape(width, width).astype(F32)).astype(BF16)
        at[...] = (clip * first[...]).astype(BF16)
        powered = base[...] + dot(gs[...], at[...], LAST_AXES)
        high, low = split(powered)
        wh[...] = high
        wl[...] = low
        wth[...] = high.T
        wtl[...] = low.T
        inner = dot(wth[...], wh[...]) + (dot(wth[...], wl[...]) + dot(wtl[...], wh[...]))
        root_h, root_l = split(inverse_root(inner, 1e-06, eye))
        qb[...] = (dot(wh[...], root_h) + (dot(wh[...], root_l) + dot(wl[...], root_h))).astype(BF16)
        qt[...] = (dot(root_h, wth[...]) + (dot(root_l, wth[...]) + dot(root_h, wtl[...]))).astype(BF16)
        ht[...] = dot(qt[...], gs[...]).astype(BF16)
        align_h, align_l = split(dot(qt[...], held))
        cross = dot(align_h, align_l, LAST_AXES)
        energy = DECAY * (dot(align_h, align_h, LAST_AXES) + (cross + cross.T)) + dot(ht[...], ht[...], LAST_AXES)
        inverse = inverse_root(energy + DAMPING * eye, 0.0, eye)
        energy_h, energy_l = split(energy)
        inverse_h, inverse_l = split(inverse)
        inner_part = dot(energy_h, inverse_h) + (dot(energy_h, inverse_l) + dot(energy_l, inverse_h))
        new[...] = dot(qb[...], inner_part.astype(BF16)).astype(BF16).reshape(npiece, prow, rank)

        def send_new(i, carry):
            t = lax.rem(f + i, nf)
            put(new.at[piece_of(t)], s_r.at[block], out_sem.at[0], out_sem.at[1], (t, r))
            return carry

        def send_up(i, carry):
            t = lax.rem(f + i, nf)
            put(up.at[t], upd_out.at[block], out_sem.at[2], out_sem.at[3], (t, r))
            return carry

        lax.fori_loop(1, nf, send_new, 0)
        mix_h, mix_l = split(math.sqrt(DAMPING) * inverse - eye)
        ft = (dot(mix_h, ht[...]) + dot(mix_l, ht[...])).astype(BF16)
        up[...] = (gs[...].astype(F32) + dot(qb[...], ft)).astype(BF16).reshape(nf, rows, width)
        lax.fori_loop(1, nf, send_up, 0)
        s_r[block] = new[piece_of(f)]
        upd_out[block] = up[f]
        wait_bytes(s_r.at[pl.ds(0, count - 1)], out_sem.at[1])

    @pl.when(jnp.logical_not(busy))
    def _():
        wait_bytes(s_r, out_sem.at[1])

    for i in range(npiece - 1, 0, -1):
        level, t = near(i, away(z))
        for q in (0, 1):
            s_x[i, q] = s_r[back[2 * t + q]]
        put(s_x.at[i], nk_out.at[:, piece_of(f)], out_sem.at[4], out_sem.at[5], (t, r))
    for q in (0, 1):
        nk_out[q, piece_of(f)] = s_r[back[2 * f + q]]

    wait_bytes(rc, send_sem.at[0])
    wait_bytes(sk_r.at[pl.ds(0, npiece - 1)], send_sem.at[1])
    wait_bytes(s_a, send_sem.at[2])
    wait_bytes(s_b, send_sem.at[3])
    wait_bytes(ss_a.at[pl.ds(0, nr - 1)], send_sem.at[5])
    wait_bytes(ss_b.at[pl.ds(0, nf - 1)], send_sem.at[7])
    wait_bytes(s_x.at[pl.ds(0, npiece - 1)], out_sem.at[4])
    wait_bytes(nk_out.at[:, pl.ds(0, npiece - 1)], out_sem.at[5])

    @pl.when(busy)
    def _():
        wait_bytes(g_out.at[pl.ds(0, count - 1)], send_sem.at[4])
        wait_bytes(z_one.at[pl.ds(0, count - 1)], send_sem.at[6])
        wait_bytes(z_one.at[pl.ds(0, nf - 1)], out_sem.at[0])
        wait_bytes(up.at[pl.ds(0, nf - 1)], out_sem.at[2])
        wait_bytes(upd_out.at[pl.ds(0, count - 1)], out_sem.at[3])

    @pl.when(jnp.logical_not(busy))
    def _():
        wait_bytes(g_out.at[pl.ds(0, count)], send_sem.at[4])
        wait_bytes(z_one.at[pl.ds(0, count)], send_sem.at[6])
        wait_bytes(upd_out, out_sem.at[3])


def finish_kernel(count, table, upd, fresh, held, upd_out, sketch_out, sem):
    first = pltpu.make_async_copy(upd, upd_out, sem.at[0])
    first.start()
    f = lax.axis_index("fsdp")
    base = lax.axis_index("rep") * count
    filled = sum(((table[base + j] == f).astype(jnp.int32) for j in range(count)), jnp.int32(0))
    for q in (0, 1):

        @pl.when(q < filled)
        def _():
            pltpu.make_async_copy(fresh.at[q], sketch_out.at[0, 0, q], sem.at[1 + q]).start()

        @pl.when(q >= filled)
        def _():
            pltpu.make_async_copy(held.at[q], sketch_out.at[0, 0, q], sem.at[1 + q]).start()

    first.wait()
    for q in (0, 1):
        pltpu.make_async_copy(fresh.at[q], sketch_out.at[0, 0, q], sem.at[1 + q]).wait()


def local(nf, nr, partials, sketch, owner_table):
    blocks_all, rows, width = partials.shape[1:]
    per_slice = blocks_all // nr
    half = per_slice // 2
    rank = sketch.shape[4]
    ny = nr // 2
    vmem = pl.BlockSpec(memory_space=pltpu.VMEM)
    anyw = pl.BlockSpec(memory_space=pl.ANY)
    hbm = pl.BlockSpec(memory_space=pltpu.HBM)
    smem = pl.BlockSpec(memory_space=pltpu.SMEM)
    dma = pltpu.SemaphoreType.DMA
    tall, wide = pltpu.VMEM((width, rank), BF16), pltpu.VMEM((rank, width), BF16)
    held = sketch[0, 0]
    table = owner_table[:, 0]
    upd, fresh = pl.pallas_call(
        functools.partial(step_kernel, nf, nr, 0.5 * math.sqrt(blocks_all * width * width)),
        out_shape=(
            jax.ShapeDtypeStruct((per_slice, rows, width), BF16),
            jax.ShapeDtypeStruct((2, nf // 2, 2 * rows, rank), BF16),
        ),
        in_specs=[hbm, hbm, hbm],
        out_specs=(vmem, vmem),
        scratch_shapes=[
            pltpu.VMEM((ny, 2, half, rows, width), BF16),
            pltpu.VMEM((ny, 2, half, rows, width), BF16),
            pltpu.VMEM((2, half, rows, width), BF16),
            pltpu.VMEM((2, half, rows, width), BF16),
            pltpu.VMEM((2, 2, half, rows, width), BF16),
            pltpu.VMEM((2, 2, half, rows, width), BF16),
            pltpu.VMEM((2, half, rows, width), BF16),
            pltpu.VMEM((nf, 2, 2 * rows, rank), BF16),
            pltpu.VMEM((per_slice, 2 * rows, rank), BF16),
            pltpu.VMEM((nr, 8, 128), F32),
            pltpu.VMEM((nf, 8, 128), F32),
            pltpu.VMEM((nf, rows, width), BF16),
            pltpu.VMEM((2, nf // 2, 2 * rows, rank), BF16),
            pltpu.VMEM((nf // 2, 2 * rows, rank), BF16),
            pltpu.VMEM((width, rank), F32),
            pltpu.VMEM((rank, width), F32),
            pltpu.VMEM((width, width), BF16),
            wide, wide, tall, tall, wide, wide, tall, wide, wide,
            pltpu.VMEM((nf, rows, width), BF16),
            pltpu.VMEM((nf // 2, 2 * rows, rank), BF16),
            pltpu.VMEM((per_slice, 2 * rows, rank), BF16),
            pltpu.VMEM((nf // 2, 2, 2 * rows, rank), BF16),
            pltpu.SMEM((per_slice,), jnp.int32),
            pltpu.SMEM((2 * nf,), jnp.int32),
            pltpu.SMEM((blocks_all,), jnp.int32),
            dma((1,)),
            dma((ny,)),
            dma((ny, half)),
            dma((2, half)),
            dma((2, 2, half)),
            dma((6,)),
            dma((8,)),
            dma((6,)),
        ],
        compiler_params=pltpu.CompilerParams(collective_id=0, has_side_effects=True, vmem_limit_bytes=48 * 2**20),
    )(table, partials.reshape(nr, 2, half, rows, width), held)

    return pl.pallas_call(
        functools.partial(finish_kernel, per_slice),
        out_shape=(
            jax.ShapeDtypeStruct((per_slice, rows, width), BF16),
            jax.ShapeDtypeStruct((1, 1, 2, width, rank), BF16),
        ),
        in_specs=[smem, vmem, vmem, vmem],
        out_specs=(anyw, anyw),
        scratch_shapes=[dma((3,))],
        compiler_params=pltpu.CompilerParams(vmem_limit_bytes=4 * 2**20),
    )(table, upd, fresh.reshape(2, width, rank), held)


def solution(mesh):
    nf, nr = mesh.shape["fsdp"], mesh.shape["rep"]
    return jax.shard_map(
        functools.partial(local, nf, nr),
        mesh=mesh,
        in_specs=(P("rep", None, "fsdp", None), P("fsdp", "rep", None, None, None), P()),
        out_specs=(P("rep", "fsdp", None), P("fsdp", "rep", None, None, None)),
        check_vma=False,
    )
```

```python
import functools
import math

import jax
import jax.numpy as jnp
from jax import lax
from jax.experimental import pallas as pl
from jax.experimental.pallas import tpu as pltpu
from jax.sharding import PartitionSpec as P

NS_ITERS = 5
DECAY = 0.9
DAMPING = 64.0
LAST_AXES = (((1,), (1,)), ((), ()))
MESH = pl.DeviceIdType.MESH
F32 = jnp.float32
BF16 = jnp.bfloat16


def dot(a, b, dims=(((1,), (0,)), ((), ()))):
    return lax.dot_general(a, b, dims, preferred_element_type=F32)


def split(value):
    high = value.astype(BF16)
    return high, (value - high.astype(F32)).astype(BF16)


def inverse_root(matrix, epsilon, eye):
    trace = jnp.sum(jnp.sum(matrix * eye, axis=1, keepdims=True), axis=0, keepdims=True) + epsilon
    state = matrix * (1.0 / trace)
    inverse = 1.5 * eye - 0.5 * state
    for step in range(1, NS_ITERS):
        low = state.astype(BF16)
        half = 1.5 * state - 0.5 * dot(low, low)
        state = 1.5 * half - 0.5 * dot(low, half.astype(BF16))
        low = state.astype(BF16)
        high_part, low_part = split(inverse)
        inverse = 1.5 * inverse - 0.5 * (dot(low, high_part) + dot(low, low_part))
    return inverse * (1.0 / jnp.sqrt(trace))


def wait_bytes(ref, sem):
    pltpu.make_async_copy(ref, ref, sem).wait()


def put(src, dst, send, recv, device):
    pltpu.make_async_remote_copy(
        src_ref=src, dst_ref=dst, send_sem=send, recv_sem=recv, device_id=device, device_id_type=MESH
    ).start()


def barrier_with(f, r, nf, nr, with_rep):
    barrier = pltpu.get_barrier_semaphore()

    def to_fsdp(i, carry):
        pl.semaphore_signal(barrier, inc=1, device_id=(lax.rem(f + i, nf), r), device_id_type=MESH)
        return carry

    def to_rep(i, carry):
        pl.semaphore_signal(barrier, inc=1, device_id=(f, lax.rem(r + i, nr)), device_id_type=MESH)
        return carry

    lax.fori_loop(1, nf, to_fsdp, 0)
    if with_rep:
        lax.fori_loop(1, nr, to_rep, 0)
    pl.semaphore_wait(barrier, nf - 1 + (nr - 1 if with_rep else 0))


def step_kernel(
    nf, nr, limit, table_in, part, sk, upd_out, nk_out,
    own, rc, s_a, r_a, s_b, r_b, fin, sk_r, sk_s, ss_a, ss_b, g_out, z_out, z_in, base, first,
    gs, zt, at, wh, wl, wth, wtl, qb, qt, ht, up, new, s_r, s_x, slots, back, table,
    tab_sem, own_sem, rc_sem, ra_sem, rb_sem, gz_sem, send_sem, out_sem,
):
    f = lax.axis_index("fsdp")
    r = lax.axis_index("rep")
    ny = nr // 2
    steps = own.shape[2]
    rows = own.shape[3]
    y = r // 2
    c = lax.rem(r, 2)
    z_one = z_out.reshape(z_out.shape[0] * z_out.shape[1], *z_out.shape[2:])
    nx, nz, npiece = 4, nf // 4, nf // 2
    prow = sk_r.shape[2]
    z, x = f // nx, lax.rem(f, nx)
    partner = (f, 2 * y + 1 - c)
    ydev = ((f, 2 * lax.rem(y + 1, ny) + c), (f, 2 * lax.rem(y + ny - 1, ny) + c))
    rel = (1, ny - 1)

    def place(j):
        n = 2 * j + c
        return n + (n + 4) // 8

    spot = f - (f + 5) // 9
    busy = (lax.rem(f + 5, 9) != 0) & (lax.rem(spot, 2) == c)
    block = spot // 2

    owners_in = pltpu.make_async_copy(table_in, table, tab_sem.at[0])
    owners_in.start()

    def far_first(send):
        hops = lambda o: min(o // nx, nz - o // nx) + min(o % nx, nx - o % nx)
        for o in sorted(range(1, nf), key=lambda o: -hops(o)):
            send(lax.rem(z + o // nx, nz) * nx + lax.rem(x + o % nx, nx))

    for d in (2, 1, 3, 0):
        pltpu.make_async_copy(part.at[2 * lax.rem(y + d, ny) + c], own.at[d], own_sem.at[d]).start()

    barrier_with(f, r, nf, nr, True)

    def order(i):
        return lax.rem(f + i, steps)

    for i in range(steps):
        k = order(i)
        for d in (2, 1, 3, 0):
            put(part.at[2 * lax.rem(y + d, ny) + 1 - c, :, k], rc.at[d, :, k], send_sem.at[0], rc_sem.at[d, k], partner)

    def away(level):
        return jnp.where(lax.rem(level, 2) == 0, 2, nz - 2)

    def near(i, two):
        level = lax.rem(z + jnp.where(i // nx == 3, two, (0, 1, nz - 1, 0)[i // nx]), nz)
        return level, level * nx + lax.rem(x + i % nx, nx)

    def piece_of(t):
        return lax.rem(t, npiece)

    def cut(t):
        return pl.ds(pl.multiple_of(piece_of(t) * prow, prow), prow)

    mine = pltpu.make_async_copy(sk.at[:, cut(f), :], sk_r.at[f], gz_sem.at[3])
    mine.start()
    for i in range(npiece - 1, 0, -1):
        level, t = near(i, nz - away(z))
        put(sk.at[:, cut(t), :], sk_r.at[f], send_sem.at[1], gz_sem.at[0], (t, r))

    count = 2 * steps
    owners_in.wait()
    owners = [table[r * count + j] for j in range(count)]
    for j in range(count):
        slots[j] = 2 * owners[j] + sum(((owners[i] == owners[j]).astype(jnp.int32) for i in range(j)), jnp.int32(0))

    def invert(t, carry):
        at = jnp.int32(0)
        for j in range(count):
            at = jnp.where(slots[j] == t, j, at)
        back[t] = at
        return carry

    lax.fori_loop(0, 2 * nf, invert, 0)

    for d in (2, 1, 3, 0):
        pltpu.make_async_copy(own.at[d], own.at[d], own_sem.at[d]).wait()

    def both(d, h, k):
        return own[d, h, k].astype(F32) + rc[d, h, k].astype(F32)

    def opposite(k):
        wait_bytes(rc.at[2, :, k], rc_sem.at[2, k])
        for d in (0, 1):
            s_a[d, k] = both(2, d, k).astype(BF16)
            put(s_a.at[d, k], r_a.at[d, k], send_sem.at[2], ra_sem.at[d, k], ydev[d])

    def independent(k):
        for d in (0, 1):
            wait_bytes(rc.at[rel[d], :, k], rc_sem.at[rel[d], k])
            s_b[d, 1 - d, k] = both(rel[d], 1 - d, k).astype(BF16)
            put(s_b.at[d, 1 - d, k], r_b.at[d, 1 - d, k], send_sem.at[3], rb_sem.at[d, 1 - d, k], ydev[d])

    def dependent(k):
        for d in (0, 1):
            wait_bytes(r_a.at[d, k], ra_sem.at[d, k])
            s_b[d, d, k] = (both(rel[d], d, k) + r_a[d, k].astype(F32)).astype(BF16)
            put(s_b.at[d, d, k], r_b.at[d, d, k], send_sem.at[3], rb_sem.at[d, d, k], ydev[d])

    def final(k, total):
        wait_bytes(rc.at[0, :, k], rc_sem.at[0, k])
        for h in (0, 1):
            wait_bytes(r_b.at[1 - h, h, k], rb_sem.at[1 - h, h, k])
            wait_bytes(r_b.at[h, h, k], rb_sem.at[h, h, k])
            value = (both(0, h, k) + (r_b[0, h, k].astype(F32) + r_b[1, h, k].astype(F32))).astype(BF16)
            fin[h, k] = value
            target = place(h * steps + k)

            @pl.when(target != f)
            def _():
                put(fin.at[h, k], g_out.at[f], send_sem.at[4], gz_sem.at[1], (target, r))

            @pl.when(target == f)
            def _():
                g_out[f] = value

            wide = value.astype(F32)
            square = wide * wide
            total = total + jnp.sum(square.reshape(rows // 8, 8, square.shape[1] // 128, 128).transpose(0, 2, 1, 3).reshape(-1, 8, 128), axis=0)
        return total

    def sketches():
        mine.wait()
        wait_bytes(sk_r.at[pl.ds(0, npiece - 1)], gz_sem.at[0])
        for i in range(2 * steps):
            j = lax.rem(f + i, 2 * steps)
            target = place(j)
            slot = slots[j]
            owner = slot // 2
            apart = lax.rem(owner // nx - z + nz, nz)
            here = (apart <= 1) | (apart == nz - 1) | (apart == away(z))
            sk_s[j] = sk_r[jnp.where(here, owner, f), lax.rem(slot, 2)]

            @pl.when(target != f)
            def _():
                put(sk_s.at[j], z_out.at[f // npiece, piece_of(f)], send_sem.at[6], gz_sem.at[2], (target, r))

            @pl.when(target == f)
            def _():
                z_out[f // npiece, piece_of(f)] = sk_s[j]

    total = jnp.zeros((8, 128), F32)
    for i in range(steps + 2):
        if i < steps:
            opposite(order(i))
        if 1 <= i < steps + 1:
            independent(order(i - 1))
        if 1 <= i < steps + 1:
            dependent(order(i - 1))
        if i == 4:
            sketches()
        if i >= 2:
            total = final(order(i - 2), total)

    ss_a[r] = total

    def rep_send(i, carry):
        put(ss_a.at[r], ss_a.at[r], send_sem.at[5], gz_sem.at[4], (f, lax.rem(r + i, nr)))
        return carry

    lax.fori_loop(1, nr, rep_send, 0)
    wait_bytes(ss_a.at[pl.ds(0, nr - 1)], gz_sem.at[4])
    ss_b[f] = jnp.sum(ss_a[...], axis=0)

    def fsdp_send(i, carry):
        put(ss_b.at[f], ss_b.at[f], send_sem.at[7], gz_sem.at[5], (lax.rem(f + i, nf), r))
        return carry

    lax.fori_loop(1, nf, fsdp_send, 0)

    width, rank = g_out.shape[2], sk_r.shape[3]

    @pl.when(busy)
    def _():
        wait_bytes(z_one.at[pl.ds(0, nf - 1)], gz_sem.at[2])
        level = slots[block] // (2 * nx)
        for k in range(nz // 2):
            apart = lax.rem(k - level + nz, nz)
            low = (apart <= 1) | (apart == nz - 1) | (apart == nz - away(level))
            z_in[k * nx : (k + 1) * nx] = z_out[jnp.where(low, 0, 1), k * nx : (k + 1) * nx]
        held = z_in[...].reshape(width, rank)
        zt[...] = held.T
        gram = dot(zt[...], held).astype(BF16)
        base[...] = DECAY * dot(held, gram)
        wait_bytes(g_out.at[pl.ds(0, nf - 1)], gz_sem.at[1])
        first[...] = dot(zt[...], g_out[...].reshape(width, width))

    wait_bytes(ss_b.at[pl.ds(0, nf - 1)], gz_sem.at[5])

    @pl.when(busy)
    def _():
        eye = (
            lax.broadcasted_iota(jnp.int32, (rank, rank), 0) == lax.broadcasted_iota(jnp.int32, (rank, rank), 1)
        ).astype(F32)
        held = z_in[...].reshape(width, rank)
        squares = jnp.sum(ss_b[...], axis=0)
        squares = jnp.sum(jnp.sum(squares, axis=1, keepdims=True), axis=0, keepdims=True)
        clip = jnp.minimum(1.0, limit / jnp.sqrt(squares + 1e-06))
        gs[...] = (clip * g_out[...].reshape(width, width).astype(F32)).astype(BF16)
        at[...] = (clip * first[...]).astype(BF16)
        powered = base[...] + dot(gs[...], at[...], LAST_AXES)
        high, low = split(powered)
        wh[...] = high
        wl[...] = low
        wth[...] = high.T
        wtl[...] = low.T
        inner = dot(wth[...], wh[...]) + (dot(wth[...], wl[...]) + dot(wtl[...], wh[...]))
        root_h, root_l = split(inverse_root(inner, 1e-06, eye))
        qb[...] = (dot(wh[...], root_h) + (dot(wh[...], root_l) + dot(wl[...], root_h))).astype(BF16)
        qt[...] = (dot(root_h, wth[...]) + (dot(root_l, wth[...]) + dot(root_h, wtl[...]))).astype(BF16)
        ht[...] = dot(qt[...], gs[...]).astype(BF16)
        align_h, align_l = split(dot(qt[...], held))
        cross = dot(align_h, align_l, LAST_AXES)
        energy = DECAY * (dot(align_h, align_h, LAST_AXES) + (cross + cross.T)) + dot(ht[...], ht[...], LAST_AXES)
        inverse = inverse_root(energy + DAMPING * eye, 0.0, eye)
        energy_h, energy_l = split(energy)
        inverse_h, inverse_l = split(inverse)
        inner_part = dot(energy_h, inverse_h) + (dot(energy_h, inverse_l) + dot(energy_l, inverse_h))
        new[...] = dot(qb[...], inner_part.astype(BF16)).astype(BF16).reshape(npiece, prow, rank)

        def send_new(t):
            put(new.at[piece_of(t)], s_r.at[block], out_sem.at[0], out_sem.at[1], (t, r))

        def send_up(t):
            put(up.at[t], upd_out.at[block], out_sem.at[2], out_sem.at[3], (t, r))

        far_first(send_new)
        mix_h, mix_l = split(math.sqrt(DAMPING) * inverse - eye)
        ft = (dot(mix_h, ht[...]) + dot(mix_l, ht[...])).astype(BF16)
        up[...] = (gs[...].astype(F32) + dot(qb[...], ft)).astype(BF16).reshape(nf, rows, width)
        lax.fori_loop(1, nf, lambda i, carry: (send_up(lax.rem(f + i, nf)), carry)[1], 0)
        s_r[block] = new[piece_of(f)]
        upd_out[block] = up[f]
        wait_bytes(s_r.at[pl.ds(0, count - 1)], out_sem.at[1])

    @pl.when(jnp.logical_not(busy))
    def _():
        wait_bytes(s_r, out_sem.at[1])

    for i in range(npiece - 1, 0, -1):
        level, t = near(i, away(z))
        for q in (0, 1):
            s_x[i, q] = s_r[back[2 * t + q]]
        put(s_x.at[i], nk_out.at[:, piece_of(f)], out_sem.at[4], out_sem.at[5], (t, r))
    for q in (0, 1):
        nk_out[q, piece_of(f)] = s_r[back[2 * f + q]]

    wait_bytes(rc, send_sem.at[0])
    wait_bytes(sk_r.at[pl.ds(0, npiece - 1)], send_sem.at[1])
    wait_bytes(s_a, send_sem.at[2])
    wait_bytes(s_b, send_sem.at[3])
    wait_bytes(ss_a.at[pl.ds(0, nr - 1)], send_sem.at[5])
    wait_bytes(ss_b.at[pl.ds(0, nf - 1)], send_sem.at[7])
    wait_bytes(s_x.at[pl.ds(0, npiece - 1)], out_sem.at[4])
    wait_bytes(nk_out.at[:, pl.ds(0, npiece - 1)], out_sem.at[5])

    @pl.when(busy)
    def _():
        wait_bytes(g_out.at[pl.ds(0, count - 1)], send_sem.at[4])
        wait_bytes(z_one.at[pl.ds(0, count - 1)], send_sem.at[6])
        wait_bytes(z_one.at[pl.ds(0, nf - 1)], out_sem.at[0])
        wait_bytes(up.at[pl.ds(0, nf - 1)], out_sem.at[2])
        wait_bytes(upd_out.at[pl.ds(0, count - 1)], out_sem.at[3])

    @pl.when(jnp.logical_not(busy))
    def _():
        wait_bytes(g_out.at[pl.ds(0, count)], send_sem.at[4])
        wait_bytes(z_one.at[pl.ds(0, count)], send_sem.at[6])
        wait_bytes(upd_out, out_sem.at[3])


def finish_kernel(count, table, upd, fresh, held, upd_out, sketch_out, sem):
    first = pltpu.make_async_copy(upd, upd_out, sem.at[0])
    first.start()
    f = lax.axis_index("fsdp")
    base = lax.axis_index("rep") * count
    filled = sum(((table[base + j] == f).astype(jnp.int32) for j in range(count)), jnp.int32(0))
    for q in (0, 1):

        @pl.when(q < filled)
        def _():
            pltpu.make_async_copy(fresh.at[q], sketch_out.at[0, 0, q], sem.at[1 + q]).start()

        @pl.when(q >= filled)
        def _():
            pltpu.make_async_copy(held.at[q], sketch_out.at[0, 0, q], sem.at[1 + q]).start()

    first.wait()
    for q in (0, 1):
        pltpu.make_async_copy(fresh.at[q], sketch_out.at[0, 0, q], sem.at[1 + q]).wait()


def local(nf, nr, partials, sketch, owner_table):
    blocks_all, rows, width = partials.shape[1:]
    per_slice = blocks_all // nr
    half = per_slice // 2
    rank = sketch.shape[4]
    ny = nr // 2
    vmem = pl.BlockSpec(memory_space=pltpu.VMEM)
    anyw = pl.BlockSpec(memory_space=pl.ANY)
    hbm = pl.BlockSpec(memory_space=pltpu.HBM)
    smem = pl.BlockSpec(memory_space=pltpu.SMEM)
    dma = pltpu.SemaphoreType.DMA
    tall, wide = pltpu.VMEM((width, rank), BF16), pltpu.VMEM((rank, width), BF16)
    held = sketch[0, 0]
    table = owner_table[:, 0]
    upd, fresh = pl.pallas_call(
        functools.partial(step_kernel, nf, nr, 0.5 * math.sqrt(blocks_all * width * width)),
        out_shape=(
            jax.ShapeDtypeStruct((per_slice, rows, width), BF16),
            jax.ShapeDtypeStruct((2, nf // 2, 2 * rows, rank), BF16),
        ),
        in_specs=[hbm, hbm, hbm],
        out_specs=(vmem, vmem),
        scratch_shapes=[
            pltpu.VMEM((ny, 2, half, rows, width), BF16),
            pltpu.VMEM((ny, 2, half, rows, width), BF16),
            pltpu.VMEM((2, half, rows, width), BF16),
            pltpu.VMEM((2, half, rows, width), BF16),
            pltpu.VMEM((2, 2, half, rows, width), BF16),
            pltpu.VMEM((2, 2, half, rows, width), BF16),
            pltpu.VMEM((2, half, rows, width), BF16),
            pltpu.VMEM((nf, 2, 2 * rows, rank), BF16),
            pltpu.VMEM((per_slice, 2 * rows, rank), BF16),
            pltpu.VMEM((nr, 8, 128), F32),
            pltpu.VMEM((nf, 8, 128), F32),
            pltpu.VMEM((nf, rows, width), BF16),
            pltpu.VMEM((2, nf // 2, 2 * rows, rank), BF16),
            pltpu.VMEM((nf // 2, 2 * rows, rank), BF16),
            pltpu.VMEM((width, rank), F32),
            pltpu.VMEM((rank, width), F32),
            pltpu.VMEM((width, width), BF16),
            wide, wide, tall, tall, wide, wide, tall, wide, wide,
            pltpu.VMEM((nf, rows, width), BF16),
            pltpu.VMEM((nf // 2, 2 * rows, rank), BF16),
            pltpu.VMEM((per_slice, 2 * rows, rank), BF16),
            pltpu.VMEM((nf // 2, 2, 2 * rows, rank), BF16),
            pltpu.SMEM((per_slice,), jnp.int32),
            pltpu.SMEM((2 * nf,), jnp.int32),
            pltpu.SMEM((blocks_all,), jnp.int32),
            dma((1,)),
            dma((ny,)),
            dma((ny, half)),
            dma((2, half)),
            dma((2, 2, half)),
            dma((6,)),
            dma((8,)),
            dma((6,)),
        ],
        compiler_params=pltpu.CompilerParams(collective_id=0, has_side_effects=True, vmem_limit_bytes=52 * 2**20),
    )(table, partials.reshape(nr, 2, half, rows, width), held)

    return pl.pallas_call(
        functools.partial(finish_kernel, per_slice),
        out_shape=(
            jax.ShapeDtypeStruct((per_slice, rows, width), BF16),
            jax.ShapeDtypeStruct((1, 1, 2, width, rank), BF16),
        ),
        in_specs=[smem, vmem, vmem, vmem],
        out_specs=(anyw, anyw),
        scratch_shapes=[dma((3,))],
        compiler_params=pltpu.CompilerParams(vmem_limit_bytes=4 * 2**20),
    )(table, upd, fresh.reshape(2, width, rank), held)


def solution(mesh):
    nf, nr = mesh.shape["fsdp"], mesh.shape["rep"]
    return jax.shard_map(
        functools.partial(local, nf, nr),
        mesh=mesh,
        in_specs=(P("rep", None, "fsdp", None), P("fsdp", "rep", None, None, None), P()),
        out_specs=(P("rep", "fsdp", None), P("fsdp", "rep", None, None, None)),
        check_vma=False,
    )
```
